256 devices in a mesh: dp: 32 (over x, y, core), tensor: 8 (over z).
Axes of the slice: x: 4, y: 4, z: 8, core: 2. Of those that a mesh axis runs over, the one named last changes fastest.
Arguments:
- img_hidden: bfloat16 [32768, 4304], P('dp', 'tensor'), may hold values from -0.25 to 0.25
- img_down: bfloat16 [4304, 1152], P('tensor'), may hold values from -0.09375 to 0.09375
- img_pooled: bfloat16 [32768, 1152], P(('dp', 'tensor')), may hold values from -0.25 to 0.25
- txt_hidden: bfloat16 [32768, 1152], P('dp', 'tensor'), may hold values from -0.25 to 0.25
- txt_proj: bfloat16 [1152, 1152], P('tensor'), may hold values from -0.1875 to 0.1875
- log_temp: float32 [1], replicated, may hold values from 1 to 2
- bias: float32 [1], replicated, may hold values from -4 to -1
- match: int32 [32768], P(('dp', 'tensor')), may hold values from 0 to 32767
- window_index: int32 [1], replicated, may hold values from 0 to 15
Outputs:
- img_grad: float32 [32768, 1152], P(('dp', 'tensor'))
- txt_grad: float32 [32768, 1152], P(('dp', 'tensor'))
- row_loss: float32 [32768], P(('dp', 'tensor'))
The draws below stay inside these ranges and needn't reach their ends.
All inputs are finite; a program needn't handle non-finite values.
Results may differ from the reference program's by a relative error of at most 0.0039.
Values may be sent and summed in bfloat16 or wider, within the bound.
No kernel may reach another device: no remote copies, remote signals or barrier semaphores. Data moves between devices by JAX's collectives and lax.ppermute only.
A program may use at most 64 MiB of HBM per device.

```python
import jax
import jax.numpy as jnp
from jax import lax

D = 1152
K_IMG = 4304
K_TXT = 1152
ROWS = 128
STEPS = 16
BATCH = 32768
WINDOWS = 16
N_DP = 32
N_TENSOR = 8


def plant(values, key, low, top_value):
    spot = [jax.random.randint(jax.random.fold_in(key, axis), (), 0, length) for axis, length in enumerate(values.shape)]
    main_axis = values.shape.index(max(values.shape))
    neighbour = spot[:main_axis] + [(spot[main_axis] + 1) % values.shape[main_axis]] + spot[main_axis + 1:]
    return values.at[tuple(spot)].set(low).at[tuple(neighbour)].set(top_value)


def block_scale(stream_key, dims, shards, smallest, largest):
    level = 1.0
    for dim, parts in shards:
        steps = jax.random.uniform(jax.random.fold_in(jax.random.fold_in(stream_key, 6), dim), (parts,), jnp.float32, smallest / len(shards), largest / len(shards))
        level = level * jnp.repeat(jnp.exp(steps), dims[dim] // parts).reshape((-1,) + (1,) * (len(dims) - 1 - dim))
    return level


def noise(rng, shape, scale, bound, split=(), kind=jnp.bfloat16):
    gain = block_scale(rng, shape, split, -0.22, 0.18) if split else 1.0
    array = jax.random.normal(rng, shape, jnp.float32) * scale * gain
    return jnp.minimum(jnp.maximum(array, -bound), bound).astype(kind)


def setup_inputs(seed: int = 0) -> dict:
    streams_of = jax.random.split(jax.random.key(seed), 10)
    img_hidden = noise(streams_of[0], (BATCH, K_IMG), 0.03125, 0.25, ((0, 32), (1, 8)))
    img_down = noise(streams_of[1], (K_IMG, D), K_IMG ** -0.5, 0.09375, ((0, 8),))
    img_pooled = noise(streams_of[2], (BATCH, D), 0.03125, 0.25, ((0, 256),))
    txt_hidden = noise(streams_of[3], (BATCH, K_TXT), 0.03125, 0.25, ((0, 32), (1, 8)))
    txt_proj = noise(streams_of[4], (K_TXT, D), K_TXT ** -0.5, 0.1875, ((0, 8),))
    log_temp = jnp.clip(jax.random.uniform(streams_of[5], (1,), jnp.float32, 1.0, 2.0), 1.0, 2.0)
    bias = jnp.clip(jax.random.uniform(streams_of[6], (1,), jnp.float32, -4.0, -1.0), -4.0, -1.0)
    match = plant(jax.random.randint(streams_of[7], (BATCH,), 0, BATCH), jax.random.fold_in(streams_of[7], 1), 0, BATCH - 1).astype(jnp.int32)
    window_index = jax.random.randint(streams_of[8], (1,), 0, WINDOWS).astype(jnp.int32)
    return {"img_hidden": img_hidden, "img_down": img_down, "img_pooled": img_pooled, "txt_hidden": txt_hidden, "txt_proj": txt_proj, "log_temp": log_temp, "bias": bias, "match": match, "window_index": window_index}


def unit_rows(emb):
    length = jnp.sqrt(lax.optimization_barrier(jnp.sum(emb * emb, axis=1, keepdims=True)) + 1e-06)
    return (emb / length, length)

def reference(img_hidden, img_down, img_pooled, txt_hidden, txt_proj, log_temp, bias, match, window_index):
    img_emb = jnp.dot(img_hidden, img_down, preferred_element_type=jnp.float32) + img_pooled.astype(jnp.float32)
    txt_emb = jnp.dot(txt_hidden, txt_proj, preferred_element_type=jnp.float32)
    img_unit, img_len = unit_rows(img_emb)
    txt_unit, txt_len = unit_rows(txt_emb)
    blocks = N_DP * N_TENSOR
    image_low = img_unit.astype(jnp.bfloat16).astype(jnp.float32).reshape(blocks, ROWS, D)
    text_low = txt_unit.astype(jnp.bfloat16).astype(jnp.float32).reshape(blocks, ROWS, D)
    scale = jnp.exp(log_temp[0])
    shift_value = bias[0]
    base = window_index[0] * STEPS
    match_blocks = match.reshape(blocks, ROWS)
    owners_base = jnp.arange(blocks, dtype=jnp.int32)
    row_offsets = jnp.arange(ROWS, dtype=jnp.int32)
    image_dunit = jnp.zeros((blocks, ROWS, D), jnp.float32)
    text_dunit = jnp.zeros((blocks, ROWS, D), jnp.float32)
    row_loss = jnp.zeros((blocks, ROWS), jnp.float32)
    for offset_step in range(STEPS):
        offset = (base + offset_step).astype(jnp.int32)
        texts = jnp.roll(text_low, offset, axis=0)
        owners = (owners_base - offset) % blocks
        text_index = owners[:, None] * ROWS + row_offsets[None, :]
        positive = match_blocks[:, :, None] == text_index[:, None, :]
        cosine = jnp.einsum('prd,pqd->prq', image_low, texts)
        logit = scale * cosine + shift_value
        row_loss = row_loss + lax.optimization_barrier(jnp.sum(jnp.where(positive, jax.nn.softplus(-logit), jax.nn.softplus(logit)), axis=2))
        coef = ((jax.nn.sigmoid(logit) - positive.astype(jnp.float32)) * scale).astype(jnp.bfloat16).astype(jnp.float32)
        image_dunit = image_dunit + jnp.einsum('prq,pqd->prd', coef, texts)
        text_dunit = text_dunit + jnp.roll(jnp.einsum('prq,prd->pqd', coef, image_low), -offset, axis=0)
    image_dunit = image_dunit.reshape(BATCH, D)
    text_dunit = text_dunit.reshape(BATCH, D)
    img_grad = (image_dunit - img_unit * lax.optimization_barrier(jnp.sum(img_unit * image_dunit, axis=1, keepdims=True))) / img_len
    txt_grad = (text_dunit - txt_unit * lax.optimization_barrier(jnp.sum(txt_unit * text_dunit, axis=1, keepdims=True))) / txt_len
    return (img_grad, txt_grad, row_loss.reshape(BATCH))
```

```python
import jax
import jax.numpy as jnp
from jax import lax
from jax.sharding import Mesh, PartitionSpec as P

STEPS = 16
ROWS_OF = ("chip", "core")
ALL = ("chip", "core", "z")


def shifted(shard, axis, by):
    devices = lax.axis_size(axis)
    return lax.ppermute(shard, axis, [(i, (i + by) % devices) for i in range(devices)])


def shifted_by_window(shard, window, sign):
    chips = lax.axis_size("chip")

    def branch(by):
        if by == 0:
            return lambda value: value
        return lambda value: shifted(value, "chip", sign * by)

    return lax.switch(window, [branch(by) for by in range(chips)], shard)


def unit_rows(emb):
    length = jnp.sqrt(jnp.sum(emb * emb, axis=1, keepdims=True) + 1e-06)
    return (emb / length, length)


def logits(rows, columns, scale, shift_value):
    cosine = lax.dot_general(
        rows, columns, (((1,), (1,)), ((), ())), preferred_element_type=jnp.float32
    )
    return scale * cosine + shift_value


def coefs(logit, positive, scale):
    return ((jax.nn.sigmoid(logit) - positive.astype(jnp.float32)) * scale).astype(jnp.bfloat16)


def body(
    img_hidden, img_down, img_pooled, txt_hidden, txt_proj, log_temp, bias, match, window_index
):
    rows = img_pooled.shape[0]
    scale = jnp.exp(log_temp[0])
    shift_value = bias[0]
    window = window_index[0]
    place = lax.axis_index(ALL)
    devices = lax.axis_size(ALL)
    z = lax.axis_index("z")
    z_size = lax.axis_size("z")
    core = lax.axis_index("core")

    half = txt_proj.shape[0] // 2
    proj_half = lax.dynamic_slice_in_dim(txt_proj, core * half, half, 0)
    proj = lax.all_gather(proj_half, ("z", "core"), axis=0, tiled=True)

    img_part = jnp.dot(img_hidden, img_down, preferred_element_type=jnp.float32)
    img_sum = lax.psum_scatter(img_part, "z", scatter_dimension=0, tiled=True)

    hidden = shifted_by_window(txt_hidden.T, window, 1)
    hidden = lax.all_gather(hidden, "z", axis=0, tiled=True)
    txt_emb = lax.dot_general(
        hidden, proj, (((0,), (0,)), ((), ())), preferred_element_type=jnp.float32
    )
    txt_unit_all, txt_len_all = unit_rows(txt_emb)
    text_0 = txt_unit_all.astype(jnp.bfloat16)
    text_1 = shifted(text_0, ROWS_OF, 1)
    text_2 = shifted(text_1, ROWS_OF, 1)

    matches = match
    for level in range(4):
        matches = jnp.concatenate([matches, shifted(matches, ALL, -(1 << level))])

    img_emb = img_sum + img_pooled.astype(jnp.float32)
    img_unit, img_len = unit_rows(img_emb)
    image_low = img_unit.astype(jnp.bfloat16)
    image_0 = lax.all_gather(image_low, "z", axis=0, tiled=True)
    image_2 = lax.all_gather(shifted(image_low, ROWS_OF, -2), "z", axis=0, tiled=True)
    image_1 = shifted(image_0, ROWS_OF, -1)

    row_iota = lax.iota(jnp.int32, z_size * rows)
    block_of = row_iota // rows
    column_base = (place - z) * rows
    total_rows = devices * rows
    window_rows = window * STEPS * rows

    text_near = jnp.where((block_of <= z)[:, None], text_0, text_2)
    near_index = column_base + row_iota - jnp.where(block_of <= z, 0, 2 * z_size * rows)
    near_index = (near_index - window_rows) % total_rows
    far_index = (column_base + row_iota - z_size * rows - window_rows) % total_rows

    def image_side(columns, index):
        positive = match[:, None] == index[None, :]
        logit = logits(image_low, columns, scale, shift_value)
        loss = jnp.sum(
            jnp.where(positive, jax.nn.softplus(-logit), jax.nn.softplus(logit)), axis=1
        )
        coef = coefs(logit, positive, scale)
        return loss, jnp.dot(coef, columns, preferred_element_type=jnp.float32)

    loss_near, part_near = image_side(text_near, near_index)
    loss_far, part_far = image_side(text_1, far_index)
    row_loss = loss_near + loss_far
    image_dunit = part_near + part_far
    img_grad = (
        image_dunit - img_unit * jnp.sum(img_unit * image_dunit, axis=1, keepdims=True)
    ) / img_len

    txt_unit = lax.dynamic_slice_in_dim(txt_unit_all, z * rows, rows, 0)
    txt_len = lax.dynamic_slice_in_dim(txt_len_all, z * rows, rows, 0)
    text_low = txt_unit.astype(jnp.bfloat16)
    own_index = (place * rows - window_rows) % total_rows + lax.iota(jnp.int32, rows)

    image_near = jnp.where((block_of >= z)[:, None], image_0, image_2)
    near_match = lax.dynamic_slice_in_dim(
        jnp.concatenate([matches, matches]), (2 * z_size - z) * rows, z_size * rows
    )
    far_match = lax.dynamic_slice_in_dim(matches, (z_size - z) * rows, z_size * rows)

    def text_side(columns, index):
        positive = own_index[:, None] == index[None, :]
        coef = coefs(logits(text_low, columns, scale, shift_value), positive, scale)
        return jnp.dot(coef, columns, preferred_element_type=jnp.float32)

    text_dunit = text_side(image_near, near_match) + text_side(image_1, far_match)
    txt_grad = (
        text_dunit - txt_unit * jnp.sum(txt_unit * text_dunit, axis=1, keepdims=True)
    ) / txt_len
    txt_grad = shifted_by_window(txt_grad, window, -1)
    return (img_grad, txt_grad, row_loss)


def solution(mesh):
    z_size = mesh.shape["tensor"]
    fine = Mesh(mesh.devices.reshape(-1, 2, z_size), ALL)
    in_specs = (
        P(ROWS_OF, "z"),
        P("z", None),
        P(ALL, None),
        P(ROWS_OF, "z"),
        P("z", None),
        P(),
        P(),
        P(ALL),
        P(),
    )
    out_specs = (P(ALL, None), P(ALL, None), P(ALL))
    return jax.shard_map(body, mesh=fine, in_specs=in_specs, out_specs=out_specs, check_vma=False)
```

```python
import jax
import jax.numpy as jnp
from jax import lax
from jax.sharding import Mesh, PartitionSpec as P

STEPS = 16
SUM_SCALE = 1024.0
ROWS_OF = ("chip", "core")
ALL = ("chip", "core", "z")


def shifted(shard, axis, by):
    devices = lax.axis_size(axis)
    return lax.ppermute(shard, axis, [(i, (i + by) % devices) for i in range(devices)])


def shifted_by_window(shards, window, sign):
    chips = lax.axis_size("chip")

    def branch(by):
        if by == 0:
            return lambda *values: values
        return lambda *values: tuple(shifted(value, "chip", sign * by) for value in values)

    return lax.switch(window, [branch(by) for by in range(chips)], *shards)


def ring_gather(block):
    half = block.shape[0] // 2
    up = down = block
    ups, downs = [], []
    for _ in range(3):
        up = shifted(up, "z", 1)
        down = shifted(down, "z", -1)
        ups.append(up)
        downs.append(down)
    far = jnp.concatenate([shifted(up[:half], "z", 1), shifted(down[half:], "z", -1)])
    return [block, *ups, far, *downs[::-1]]


def ring_sum(parts, z):
    size = parts.shape[0]
    half = parts.shape[1] // 2

    def mine(ahead):
        return lax.dynamic_index_in_dim(parts, (z + ahead) % size, 0, False)

    def sent(value, by):
        return shifted(value.astype(jnp.float16), "z", by).astype(jnp.float32)

    far = mine(size // 2)
    near_up, near_down = mine(size // 2 - 1), mine(-(size // 2 - 1))
    up = jnp.concatenate([near_up[:half] + sent(far[:half], 1), near_up[half:]])
    down = jnp.concatenate([near_down[:half], near_down[half:] + sent(far[half:], -1)])
    for ahead in range(size // 2 - 2, 0, -1):
        up = mine(ahead) + sent(up, 1)
        down = mine(-ahead) + sent(down, -1)
    return mine(0) + sent(up, 1) + sent(down, -1)


def unit_rows(emb):
    length = jnp.sqrt(jnp.sum(emb * emb, axis=1, keepdims=True) + 1e-06)
    return (emb / length, length)


def logits(rows, columns, scale, shift_value):
    cosine = lax.dot_general(
        rows, columns, (((1,), (1,)), ((), ())), preferred_element_type=jnp.float32
    )
    return scale * cosine + shift_value


def coefs(logit, positive, scale):
    return ((jax.nn.sigmoid(logit) - positive.astype(jnp.float32)) * scale).astype(jnp.bfloat16)


def body(
    img_hidden, img_down, img_pooled, txt_hidden, txt_proj, log_temp, bias, match, window_index
):
    rows, width = img_pooled.shape
    scale = jnp.exp(log_temp[0])
    shift_value = bias[0]
    window = window_index[0]
    place = lax.axis_index(ALL)
    devices = lax.axis_size(ALL)
    z = lax.axis_index("z")
    z_size = lax.axis_size("z")
    core = lax.axis_index("core")
    column = z_size * rows
    total_rows = devices * rows
    window_rows = window * STEPS * rows

    img_part = jnp.dot(img_hidden, img_down, preferred_element_type=jnp.float32) * SUM_SCALE
    img_sum = ring_sum(img_part.reshape(z_size, rows, width), z) * (1.0 / SUM_SCALE)

    features = txt_proj.shape[0]
    half = features // 2
    (hidden,) = shifted_by_window((txt_hidden.T,), window, 1)
    proj_half = lax.dynamic_slice_in_dim(txt_proj, core * half, half, 0)
    payload = jnp.concatenate([hidden, proj_half.reshape(-1, column)])
    got = ring_gather(payload)
    hidden = jnp.concatenate([piece[:features] for piece in got])
    proj_mine = jnp.stack([piece[features:].reshape(half, width) for piece in got])
    proj_other = shifted(proj_mine, "core", 1)
    proj = jnp.stack(
        [
            jnp.where(core == 0, proj_mine, proj_other),
            jnp.where(core == 0, proj_other, proj_mine),
        ],
        axis=1,
    ).reshape(-1, width)
    txt_emb = lax.dot_general(
        hidden, proj, (((0,), (0,)), ((), ())), preferred_element_type=jnp.float32
    )
    txt_unit_all, txt_len_all = unit_rows(txt_emb)
    text_here = txt_unit_all.astype(jnp.bfloat16)
    text_before = shifted(text_here, "chip", 1)

    matches = match
    for level in range(4):
        matches = jnp.concatenate([matches, shifted(matches, ALL, -(1 << level))])
    match_other = shifted(match, "core", 1)

    img_emb = img_sum + img_pooled.astype(jnp.float32)
    img_unit, img_len = unit_rows(img_emb)
    image_low = img_unit.astype(jnp.bfloat16)
    image_other = shifted(image_low, "core", 1)
    images_here = ring_gather(image_low)
    images_after = ring_gather(shifted(image_low, "chip", -1))

    row_iota = lax.iota(jnp.int32, column)
    block_of = row_iota // rows
    column_base = (place - z) * rows

    is_here = block_of <= z
    text_near = jnp.where(is_here[:, None], text_here, text_before)
    near_index = column_base + row_iota - jnp.where(is_here, 0, 2 * column)
    near_index = (near_index - window_rows) % total_rows
    text_far = jnp.where(core == 0, text_here, text_before)
    far_index = column_base + row_iota - jnp.where(core == 0, 0, 2 * column)
    far_index = (far_index - window_rows) % total_rows

    def image_side(images, image_match, columns, index):
        positive = image_match[:, None] == index[None, :]
        logit = logits(images, columns, scale, shift_value)
        loss = jnp.sum(
            jnp.where(positive, jax.nn.softplus(-logit), jax.nn.softplus(logit)), axis=1
        )
        coef = coefs(logit, positive, scale)
        return loss, jnp.dot(coef, columns, preferred_element_type=jnp.float32)

    loss_near, part_near = image_side(image_low, match, text_near, near_index)
    loss_far, part_far = image_side(image_other, match_other, text_far, far_index)
    row_loss = loss_near + shifted(loss_far, "core", 1)
    image_dunit = part_near + shifted(part_far, "core", 1)
    img_grad = (
        image_dunit - img_unit * jnp.sum(img_unit * image_dunit, axis=1, keepdims=True)
    ) / img_len

    txt_unit = lax.dynamic_slice_in_dim(txt_unit_all, z * rows, rows, 0)
    txt_len = lax.dynamic_slice_in_dim(txt_len_all, z * rows, rows, 0)
    text_low = txt_unit.astype(jnp.bfloat16)
    text_other = shifted(text_low, "core", 1)
    own_index = (place * rows - window_rows) % total_rows + lax.iota(jnp.int32, rows)
    other_place = place + jnp.where(core == 0, z_size, -z_size)
    other_index = (other_place * rows - window_rows) % total_rows + lax.iota(jnp.int32, rows)

    source = (z - lax.iota(jnp.int32, z_size)) % z_size
    stays = source >= z
    image_near = jnp.concatenate(
        [
            jnp.where(stays[i], here, after)
            for i, (here, after) in enumerate(zip(images_here, images_after))
        ]
    )
    image_far = jnp.where(
        core == 0, jnp.concatenate(images_after), jnp.concatenate(images_here)
    )
    match_rows = matches.reshape(2 * z_size, rows)
    near_match = match_rows[(source - z) % (2 * z_size)].reshape(-1)
    far_match = shifted(match_rows[source - z + z_size].reshape(-1), "core", 1)

    def text_side(texts, text_index, columns, index):
        positive = text_index[:, None] == index[None, :]
        coef = coefs(logits(texts, columns, scale, shift_value), positive, scale)
        return jnp.dot(coef, columns, preferred_element_type=jnp.float32)

    text_far_part = text_side(text_other, other_index, image_far, far_match)
    text_near_part = text_side(text_low, own_index, image_near, near_match)
    text_dunit = text_near_part + shifted(text_far_part, "core", 1)
    tangent = text_dunit - txt_unit * jnp.sum(txt_unit * text_dunit, axis=1, keepdims=True)
    tangent, txt_len = shifted_by_window(
        (tangent.astype(jnp.float16), txt_len[:, 0]), window, -1
    )
    txt_grad = tangent.astype(jnp.float32) / txt_len[:, None]
    return (img_grad, txt_grad, row_loss)


def solution(mesh):
    z_size = mesh.shape["tensor"]
    fine = Mesh(mesh.devices.reshape(-1, 2, z_size), ALL)
    in_specs = (
        P(ROWS_OF, "z"),
        P("z", None),
        P(ALL, None),
        P(ROWS_OF, "z"),
        P("z", None),
        P(),
        P(),
        P(ALL),
        P(),
    )
    out_specs = (P(ALL, None), P(ALL, None), P(ALL))
    return jax.shard_map(body, mesh=fine, in_specs=in_specs, out_specs=out_specs, check_vma=False)
```

```python
import jax
import jax.numpy as jnp
from jax import lax
from jax.sharding import Mesh, PartitionSpec as P

STEPS = 16
SUM_SCALE = 1024.0
LOW_SCALE = 2048.0
EXTRA = 8
ROWS_OF = ("chip", "core")
ALL = ("chip", "core", "z")


def shifted(shard, axis, by):
    devices = lax.axis_size(axis)
    return lax.ppermute(shard, axis, [(i, (i + by) % devices) for i in range(devices)])


def shifted_by_window(shard, window, sign):
    chips = lax.axis_size("chip")

    def branch(by):
        if by == 0:
            return lambda value: value
        return lambda value: shifted(value, "chip", sign * by)

    return lax.switch(window, [branch(by) for by in range(chips)], shard)


def with_rows(block, *vectors):
    row = jnp.concatenate(vectors)[None, :].astype(block.dtype)
    return jnp.concatenate(
        [block, jnp.pad(row, ((0, EXTRA - 1), (0, block.shape[1] - row.shape[1])))]
    )


def ring_gather(block):
    up = down = block
    ups, downs = [], []
    for _ in range(3):
        down = shifted(down, "z", -1)
        up = shifted(up, "z", 1)
        ups.append(up)
        downs.append(down)
    return [block, *ups, shifted(down, "z", -1), *downs[::-1]]


def ring_sum(parts, z):
    size = parts.shape[0]

    def mine(ahead):
        return lax.dynamic_index_in_dim(parts, (z + ahead) % size, 0, False)

    def sent(value, by):
        return shifted(value.astype(jnp.float16), "z", by).astype(jnp.float32)

    up = mine(size // 2)
    down = None
    for ahead in range(size // 2 - 1, 0, -1):
        up = mine(ahead) + sent(up, 1)
        down = mine(-ahead) if down is None else mine(-ahead) + sent(down, -1)
    return mine(0) + sent(up, 1) + sent(down, -1)


def unit_rows(emb):
    length = jnp.sqrt(jnp.sum(emb * emb, axis=1, keepdims=True) + 1e-06)
    return (emb / length, length)


def logits(rows, columns, scale, shift_value):
    cosine = lax.dot_general(
        rows, columns, (((1,), (1,)), ((), ())), preferred_element_type=jnp.float32
    )
    return scale * cosine + shift_value


def coefs(logit, positive, scale):
    return ((jax.nn.sigmoid(logit) - positive.astype(jnp.float32)) * scale).astype(jnp.bfloat16)


def body(
    img_hidden, img_down, img_pooled, txt_hidden, txt_proj, log_temp, bias, match, window_index
):
    rows, width = img_pooled.shape
    scale = jnp.exp(log_temp[0])
    shift_value = bias[0]
    window = window_index[0]
    place = lax.axis_index(ALL)
    devices = lax.axis_size(ALL)
    z = lax.axis_index("z")
    z_size = lax.axis_size("z")
    core = lax.axis_index("core")
    column = z_size * rows
    total_rows = devices * rows
    window_rows = window * STEPS * rows

    img_part = jnp.dot(img_hidden, img_down, preferred_element_type=jnp.float32) * SUM_SCALE
    img_sum = ring_sum(img_part.reshape(z_size, rows, width), z) * (1.0 / SUM_SCALE)

    half = width // 2
    hidden = shifted_by_window(txt_hidden.T, window, 1)
    proj_half = jnp.where(core == 0, txt_proj[:, :half], txt_proj[:, half:])
    gathered = jnp.concatenate(ring_gather(jnp.concatenate([hidden, proj_half], axis=1)))
    proj_mine = gathered[:, column:]
    proj_other = shifted(proj_mine, "core", 1)
    proj = jnp.concatenate(
        [
            jnp.where(core == 0, proj_mine, proj_other),
            jnp.where(core == 0, proj_other, proj_mine),
        ],
        axis=1,
    )
    txt_emb = lax.dot_general(
        gathered[:, :column],
        proj,
        (((0,), (0,)), ((), ())),
        preferred_element_type=jnp.float32,
    )
    text_here = unit_rows(txt_emb)[0].astype(jnp.bfloat16)
    text_before = shifted(text_here, "chip", 1)

    img_emb = img_sum + img_pooled.astype(jnp.float32)
    img_unit, img_len = unit_rows(img_emb)
    image_low = img_unit.astype(jnp.bfloat16)
    block = with_rows(image_low, match // rows, match % rows)
    block_other = shifted(block, "core", 1)

    after = {0: shifted(block, "chip", -1)}
    here = {0: block, 1: shifted(block, "z", 1), -1: shifted(block, "z", -1)}
    up = jnp.stack([here[1], after[0]])
    down = jnp.stack([here[-1], after[0]])
    for step in (2, 3, 4):
        up = shifted(up, "z", 1)
        here[step], after[step - 1] = up[0], up[1]
        if step < 4:
            down = shifted(down, "z", -1)
            here[-step], after[1 - step] = down[0], down[1]
    after[-3] = shifted(after[-2], "z", -1)
    after[4] = shifted(after[-3], "z", -1)

    row_iota = lax.iota(jnp.int32, column)
    block_of = row_iota // rows
    column_base = (place - z) * rows

    is_here = block_of <= z
    text_near = jnp.where(is_here[:, None], text_here, text_before)
    near_index = column_base + row_iota - jnp.where(is_here, 0, 2 * column)
    near_index = (near_index - window_rows) % total_rows
    text_far = jnp.where(core == 0, text_here, text_before)
    far_index = column_base + row_iota - jnp.where(core == 0, 0, 2 * column)
    far_index = (far_index - window_rows) % total_rows

    def matches(blocks):
        digits = [piece[rows].astype(jnp.float32) for piece in blocks]
        return jnp.concatenate([row[:rows] * rows + row[rows : 2 * rows] for row in digits])

    def is_match(row_values, column_values):
        return row_values[:, None] == column_values.astype(jnp.float32)[None, :]

    def image_side(images, image_match, columns, index):
        positive = is_match(image_match, index)
        logit = logits(images, columns, scale, shift_value)
        loss = jnp.sum(
            jnp.where(positive, jax.nn.softplus(-logit), jax.nn.softplus(logit)), axis=1
        )
        coef = coefs(logit, positive, scale)
        return loss, jnp.dot(coef, columns, preferred_element_type=jnp.float32)

    loss_near, part_near = image_side(image_low, match.astype(jnp.float32), text_near, near_index)
    loss_far, part_far = image_side(
        block_other[:rows], matches([block_other]), text_far, far_index
    )
    row_loss = loss_near + shifted(loss_far, "core", 1)
    image_dunit = part_near + shifted(part_far, "core", 1)
    img_grad = (
        image_dunit - img_unit * jnp.sum(img_unit * image_dunit, axis=1, keepdims=True)
    ) / img_len

    txt_unit, txt_len = unit_rows(lax.dynamic_slice_in_dim(txt_emb, z * rows, rows, 0))
    text_low = txt_unit.astype(jnp.bfloat16)
    text_other = shifted(text_low, "core", 1)
    own_index = (place * rows - window_rows) % total_rows + lax.iota(jnp.int32, rows)
    other_place = place + jnp.where(core == 0, z_size, -z_size)
    other_index = (other_place * rows - window_rows) % total_rows + lax.iota(jnp.int32, rows)

    def text_side(texts, text_index, blocks):
        columns = jnp.concatenate([piece[:rows] for piece in blocks])
        positive = is_match(text_index.astype(jnp.float32), matches(blocks))
        coef = coefs(logits(texts, columns, scale, shift_value), positive, scale)
        return jnp.dot(coef, columns, preferred_element_type=jnp.float32)

    near_part = far_part = 0.0
    for group in ((0, 1, -1, 2, -2), (3, -3, 4)):
        near = [jnp.where((z - d) % z_size >= z, here[d], after[d]) for d in group]
        far = [jnp.where(core == 0, after[d], here[d]) for d in group]
        near_part = near_part + text_side(text_low, own_index, near)
        far_part = far_part + text_side(text_other, other_index, far)
    text_dunit = near_part + shifted(far_part, "core", 1)
    tangent = text_dunit - txt_unit * jnp.sum(txt_unit * text_dunit, axis=1, keepdims=True)
    len_high = txt_len[:, 0].astype(jnp.float16)
    len_low = (txt_len[:, 0] - len_high.astype(jnp.float32)) * LOW_SCALE
    home = shifted_by_window(
        with_rows(tangent.astype(jnp.float16), len_high, len_low.astype(jnp.float16)), window, -1
    ).astype(jnp.float32)
    home_len = home[rows, :rows] + home[rows, rows : 2 * rows] * (1.0 / LOW_SCALE)
    txt_grad = home[:rows] / home_len[:, None]
    return (img_grad, txt_grad, row_loss)


def solution(mesh):
    z_size = mesh.shape["tensor"]
    fine = Mesh(mesh.devices.reshape(-1, 2, z_size), ALL)
    in_specs = (
        P(ROWS_OF, "z"),
        P("z", None),
        P(ALL, None),
        P(ROWS_OF, "z"),
        P("z", None),
        P(),
        P(),
        P(ALL),
        P(),
    )
    out_specs = (P(ALL, None), P(ALL, None), P(ALL))
    return jax.shard_map(body, mesh=fine, in_specs=in_specs, out_specs=out_specs, check_vma=False)
```

```python
import jax
import jax.numpy as jnp
from jax import lax
from jax.sharding import Mesh, PartitionSpec as P

SUM_SCALE = 1024.0
LOW_SCALE = 2048.0
EXTRA = 8
LANES = 128
ROWS_OF = ("chip", "core")
ALL = ("chip", "core", "z")


def shifted(shard, axis, by):
    devices = lax.axis_size(axis)
    return lax.ppermute(shard, axis, [(i, (i + by) % devices) for i in range(devices)])


def shifted_by_window(shard, window, sign):
    chips = lax.axis_size("chip")

    def branch(by):
        if by == 0:
            return lambda value: value
        return lambda value: shifted(value, "chip", sign * by)

    return lax.switch(window, [branch(by) for by in range(chips)], shard)


def with_rows(block, *vectors):
    row = jnp.concatenate(vectors)[None, :].astype(block.dtype)
    return jnp.concatenate(
        [block, jnp.pad(row, ((0, EXTRA - 1), (0, block.shape[1] - row.shape[1])))]
    )


def ring_gather(block):
    up = down = block
    found = [block]
    for _ in range(3):
        up = shifted(up, "z", 1)
        down = shifted(down, "z", -1)
        found += [up, down]
    return [*found, shifted(down, "z", -1)]


def ring_sum(parts, z):
    size = parts.shape[0]

    def mine(ahead):
        return lax.dynamic_index_in_dim(parts, (z + ahead) % size, 0, False)

    def sent(value, by):
        return shifted(value.astype(jnp.float16), "z", by).astype(jnp.float32)

    up = mine(size // 2)
    down = None
    for ahead in range(size // 2 - 1, 0, -1):
        up = mine(ahead) + sent(up, 1)
        down = mine(-ahead) if down is None else mine(-ahead) + sent(down, -1)
    return mine(0) + sent(up, 1) + sent(down, -1)


def digits(value):
    high = value.astype(jnp.float16)
    return high, ((value - high.astype(jnp.float32)) * LOW_SCALE).astype(jnp.float16)


def unit_rows(emb):
    length = jnp.sqrt(jnp.sum(emb * emb, axis=1, keepdims=True) + 1e-06)
    return (emb / length, length)


def logits(rows, columns, scale, shift_value):
    cosine = lax.dot_general(
        rows, columns, (((1,), (1,)), ((), ())), preferred_element_type=jnp.float32
    )
    return scale * cosine + shift_value


def coefs(logit, positive, scale):
    return ((jax.nn.sigmoid(logit) - positive.astype(jnp.float32)) * scale).astype(jnp.bfloat16)


def body(
    img_hidden, img_down, img_pooled, txt_hidden, txt_proj, log_temp, bias, match, window_index
):
    rows, width = img_pooled.shape
    scale = jnp.exp(log_temp[0])
    shift_value = bias[0]
    window = window_index[0]
    place = lax.axis_index(ALL)
    devices = lax.axis_size(ALL)
    z = lax.axis_index("z")
    z_size = lax.axis_size("z")
    core = lax.axis_index("core")
    column = z_size * rows
    total_rows = devices * rows

    img_part = jnp.dot(img_hidden, img_down, preferred_element_type=jnp.float32) * SUM_SCALE
    img_sum = ring_sum(img_part.reshape(z_size, rows, width), z) * (1.0 / SUM_SCALE)

    part = (width + LANES) // 2
    features = txt_hidden.shape[1]
    proj_part = jnp.where(core == 0, txt_proj[:, :part], txt_proj[:, width - part :])
    pieces = ring_gather(jnp.concatenate([txt_hidden.T, proj_part], axis=1))
    first, second = pieces[:3], pieces[3:]
    here_first = jnp.concatenate([piece[:, :column] for piece in first])
    here_second = jnp.concatenate([piece[:, :column] for piece in second])
    before_first = shifted(here_first, "chip", 1)
    before_second = shifted(here_second, "chip", 1)
    proj_mine = jnp.concatenate([piece[:, column:] for piece in pieces])
    proj_other = shifted(proj_mine, "core", 1)
    proj = jnp.concatenate(
        [
            jnp.where(core == 0, proj_mine, proj_other),
            jnp.where(core == 0, proj_other, proj_mine)[:, 2 * part - width :],
        ],
        axis=1,
    )
    split = len(first) * features

    def text_head(hidden_first, hidden_second):
        over_features = (((0,), (0,)), ((), ()))
        return lax.dot_general(
            hidden_first, proj[:split], over_features, preferred_element_type=jnp.float32
        ) + lax.dot_general(
            hidden_second, proj[split:], over_features, preferred_element_type=jnp.float32
        )

    txt_emb = text_head(here_first, here_second)
    text_here = unit_rows(txt_emb)[0].astype(jnp.bfloat16)
    text_before = unit_rows(text_head(before_first, before_second))[0].astype(jnp.bfloat16)

    img_emb = img_sum + img_pooled.astype(jnp.float32)
    img_unit, img_len = unit_rows(img_emb)
    image_low = img_unit.astype(jnp.bfloat16)
    block = with_rows(image_low, match // rows, match % rows)
    block = shifted_by_window(block, window, -1)
    block_other = shifted(block, "core", 1)

    after = {0: shifted(block, "chip", -1)}
    here = {0: block, 1: shifted(block, "z", 1), -1: shifted(block, "z", -1)}
    up = jnp.stack([here[1], after[0]])
    down = jnp.stack([here[-1], after[0]])
    for step in (2, 3, 4):
        up = shifted(up, "z", 1)
        here[step], after[step - 1] = up[0], up[1]
        if step < 4:
            down = shifted(down, "z", -1)
            here[-step], after[1 - step] = down[0], down[1]
    after[-3] = shifted(after[-2], "z", -1)
    after[4] = shifted(after[-3], "z", -1)

    row_iota = lax.iota(jnp.int32, column)
    block_of = row_iota // rows
    column_base = (place - z) * rows

    is_here = block_of <= z
    text_near = jnp.where(is_here[:, None], text_here, text_before)
    near_index = column_base + row_iota - jnp.where(is_here, 0, 2 * column)
    near_index = near_index % total_rows
    text_far = jnp.where(core == 0, text_here, text_before)
    far_index = column_base + row_iota - jnp.where(core == 0, 0, 2 * column)
    far_index = far_index % total_rows

    def matches(blocks):
        found = [piece[rows].astype(jnp.float32) for piece in blocks]
        return jnp.concatenate([row[:rows] * rows + row[rows : 2 * rows] for row in found])

    def is_match(row_values, column_values):
        return row_values[:, None] == column_values.astype(jnp.float32)[None, :]

    def image_side(images, image_match, columns, index):
        positive = is_match(image_match, index)
        logit = logits(images, columns, scale, shift_value)
        loss = jnp.sum(
            jnp.where(positive, jax.nn.softplus(-logit), jax.nn.softplus(logit)), axis=1
        )
        coef = coefs(logit, positive, scale)
        return loss, jnp.dot(coef, columns, preferred_element_type=jnp.float32)

    met = block[:rows]
    loss_near, part_near = image_side(met, matches([block]), text_near, near_index)
    loss_far, part_far = image_side(
        block_other[:rows], matches([block_other]), text_far, far_index
    )
    met_loss = loss_near + shifted(loss_far, "core", 1)
    met_dunit = part_near + shifted(part_far, "core", 1)
    met_low = met.astype(jnp.float32)
    along = jnp.sum(met_low * met_dunit, axis=1)
    across = (met_dunit - met_low * along[:, None]).astype(jnp.float16)
    home = shifted_by_window(with_rows(across, *digits(along), *digits(met_loss)), window, 1)
    home = home.astype(jnp.float32)
    tail = home[rows]
    along = tail[:rows] + tail[rows : 2 * rows] * (1.0 / LOW_SCALE)
    row_loss = tail[2 * rows : 3 * rows] + tail[3 * rows : 4 * rows] * (1.0 / LOW_SCALE)
    image_dunit = home[:rows] + image_low.astype(jnp.float32) * along[:, None]
    img_grad = (
        image_dunit - img_unit * jnp.sum(img_unit * image_dunit, axis=1, keepdims=True)
    ) / img_len

    txt_unit, txt_len = unit_rows(lax.dynamic_slice_in_dim(txt_emb, z * rows, rows, 0))
    text_low = txt_unit.astype(jnp.bfloat16)
    text_other = shifted(text_low, "core", 1)
    own_index = place * rows + lax.iota(jnp.int32, rows)
    other_place = place + jnp.where(core == 0, z_size, -z_size)
    other_index = other_place * rows + lax.iota(jnp.int32, rows)

    def text_side(texts, text_index, blocks):
        columns = jnp.concatenate([piece[:rows] for piece in blocks])
        positive = is_match(text_index.astype(jnp.float32), matches(blocks))
        coef = coefs(logits(texts, columns, scale, shift_value), positive, scale)
        return jnp.dot(coef, columns, preferred_element_type=jnp.float32)

    near_part = far_part = 0.0
    for group in ((0, 1, -1, 2, -2), (3, -3, 4)):
        near = [jnp.where((z - d) % z_size >= z, here[d], after[d]) for d in group]
        far = [jnp.where(core == 0, after[d], here[d]) for d in group]
        near_part = near_part + text_side(text_low, own_index, near)
        far_part = far_part + text_side(text_other, other_index, far)
    text_dunit = near_part + shifted(far_part, "core", 1)
    txt_grad = (
        text_dunit - txt_unit * jnp.sum(txt_unit * text_dunit, axis=1, keepdims=True)
    ) / txt_len
    return (img_grad, txt_grad, row_loss)


def solution(mesh):
    z_size = mesh.shape["tensor"]
    fine = Mesh(mesh.devices.reshape(-1, 2, z_size), ALL)
    in_specs = (
        P(ROWS_OF, "z"),
        P("z", None),
        P(ALL, None),
        P(ROWS_OF, "z"),
        P("z", None),
        P(),
        P(),
        P(ALL),
        P(),
    )
    out_specs = (P(ALL, None), P(ALL, None), P(ALL))
    return jax.shard_map(body, mesh=fine, in_specs=in_specs, out_specs=out_specs, check_vma=False)
```

```python
import jax
import jax.numpy as jnp
from jax import lax
from jax.sharding import Mesh, PartitionSpec as P

SUM_SCALE = 1024.0
LOW_SCALE = 2048.0
EXTRA = 8
LANES = 128
ROWS_OF = ("chip", "core")
ALL = ("chip", "core", "z")


def shifted(shard, axis, by):
    devices = lax.axis_size(axis)
    return lax.ppermute(shard, axis, [(i, (i + by) % devices) for i in range(devices)])


def shifted_by_window(shard, window, sign):
    chips = lax.axis_size("chip")

    def branch(by):
        if by == 0:
            return lambda value: value
        return lambda value: shifted(value, "chip", sign * by)

    return lax.switch(window, [branch(by) for by in range(chips)], shard)


def with_rows(block, *vectors):
    row = jnp.concatenate(vectors)[None, :].astype(block.dtype)
    return jnp.concatenate(
        [block, jnp.pad(row, ((0, EXTRA - 1), (0, block.shape[1] - row.shape[1])))]
    )


def ring_gather(block):
    up = down = block
    found = [block]
    for _ in range(3):
        up = shifted(up, "z", 1)
        down = shifted(down, "z", -1)
        found += [up, down]
    return [*found, shifted(down, "z", -1)]


def ring_sum(parts, z):
    size = parts.shape[0]

    def mine(ahead):
        return lax.dynamic_index_in_dim(parts, (z + ahead) % size, 0, False)

    def sent(value, by):
        return shifted(value.astype(jnp.float16), "z", by).astype(jnp.float32)

    up = mine(size // 2)
    down = None
    for ahead in range(size // 2 - 1, 0, -1):
        up = mine(ahead) + sent(up, 1)
        down = mine(-ahead) if down is None else mine(-ahead) + sent(down, -1)
    return mine(0) + sent(up, 1) + sent(down, -1)


def digits(value):
    high = value.astype(jnp.float16)
    return high, ((value - high.astype(jnp.float32)) * LOW_SCALE).astype(jnp.float16)


def unit_rows(emb):
    length = jnp.sqrt(jnp.sum(emb * emb, axis=1, keepdims=True) + 1e-06)
    return (emb / length, length)


def logits(rows, columns, scale, shift_value):
    cosine = lax.dot_general(
        rows, columns, (((1,), (1,)), ((), ())), preferred_element_type=jnp.float32
    )
    return scale * cosine + shift_value


def coefs(logit, positive, scale):
    return ((jax.nn.sigmoid(logit) - positive.astype(jnp.float32)) * scale).astype(jnp.bfloat16)


def body(
    img_hidden, img_down, img_pooled, txt_hidden, txt_proj, log_temp, bias, match, window_index
):
    rows, width = img_pooled.shape
    scale = jnp.exp(log_temp[0])
    shift_value = bias[0]
    window = window_index[0]
    place = lax.axis_index(ALL)
    devices = lax.axis_size(ALL)
    z = lax.axis_index("z")
    z_size = lax.axis_size("z")
    core = lax.axis_index("core")
    column = z_size * rows
    total_rows = devices * rows

    img_part = jnp.dot(img_hidden, img_down, preferred_element_type=jnp.float32) * SUM_SCALE
    img_sum = ring_sum(img_part.reshape(z_size, rows, width), z) * (1.0 / SUM_SCALE)

    part = (width + LANES) // 2
    features = txt_hidden.shape[1]
    proj_part = jnp.where(core == 0, txt_proj[:, :part], txt_proj[:, width - part :])
    pieces = ring_gather(jnp.concatenate([txt_hidden.T, proj_part], axis=1))
    first, second = pieces[:5], pieces[5:]
    here_first = jnp.concatenate([piece[:, :column] for piece in first])
    here_second = jnp.concatenate([piece[:, :column] for piece in second])
    before_first = shifted(here_first, "chip", 1)
    proj_mine = jnp.concatenate([piece[:, column:] for piece in pieces])
    proj_other = shifted(proj_mine, "core", 1)
    proj = jnp.concatenate(
        [
            jnp.where(core == 0, proj_mine, proj_other),
            jnp.where(core == 0, proj_other, proj_mine)[:, 2 * part - width :],
        ],
        axis=1,
    )
    split = len(first) * features

    def text_head(hidden_first, hidden_second):
        over_features = (((0,), (0,)), ((), ()))
        return lax.dot_general(
            hidden_first, proj[:split], over_features, preferred_element_type=jnp.float32
        ) + lax.dot_general(
            hidden_second, proj[split:], over_features, preferred_element_type=jnp.float32
        )

    img_emb = img_sum + img_pooled.astype(jnp.float32)
    img_unit, img_len = unit_rows(img_emb)
    image_low = img_unit.astype(jnp.bfloat16)
    block = with_rows(image_low, match // rows, match % rows)
    block = shifted_by_window(block, window, -1)
    block, here_second = lax.optimization_barrier((block, here_second))
    before_second = shifted(here_second, "chip", 1)

    txt_emb = text_head(here_first, here_second)
    text_here = unit_rows(txt_emb)[0].astype(jnp.bfloat16)
    text_before = unit_rows(text_head(before_first, before_second))[0].astype(jnp.bfloat16)

    block_other = shifted(block, "core", 1)

    after = {0: shifted(block, "chip", -1)}
    here = {0: block, 1: shifted(block, "z", 1), -1: shifted(block, "z", -1)}
    up = jnp.stack([here[1], after[0]])
    down = jnp.stack([here[-1], after[0]])
    for step in (2, 3, 4):
        up = shifted(up, "z", 1)
        here[step], after[step - 1] = up[0], up[1]
        if step < 4:
            down = shifted(down, "z", -1)
            here[-step], after[1 - step] = down[0], down[1]
    after[-3] = shifted(after[-2], "z", -1)
    after[4] = shifted(after[-3], "z", -1)

    row_iota = lax.iota(jnp.int32, column)
    block_of = row_iota // rows
    column_base = (place - z) * rows

    is_here = block_of <= z
    text_near = jnp.where(is_here[:, None], text_here, text_before)
    near_index = column_base + row_iota - jnp.where(is_here, 0, 2 * column)
    near_index = near_index % total_rows
    text_far = jnp.where(core == 0, text_here, text_before)
    far_index = column_base + row_iota - jnp.where(core == 0, 0, 2 * column)
    far_index = far_index % total_rows

    def matches(blocks):
        found = [piece[rows].astype(jnp.float32) for piece in blocks]
        return jnp.concatenate([row[:rows] * rows + row[rows : 2 * rows] for row in found])

    def is_match(row_values, column_values):
        return row_values[:, None] == column_values.astype(jnp.float32)[None, :]

    def image_side(images, image_match, columns, index):
        positive = is_match(image_match, index)
        logit = logits(images, columns, scale, shift_value)
        loss = jnp.sum(
            jnp.where(positive, jax.nn.softplus(-logit), jax.nn.softplus(logit)), axis=1
        )
        coef = coefs(logit, positive, scale)
        return loss, jnp.dot(coef, columns, preferred_element_type=jnp.float32)

    met = block[:rows]
    loss_near, part_near = image_side(met, matches([block]), text_near, near_index)
    loss_far, part_far = image_side(
        block_other[:rows], matches([block_other]), text_far, far_index
    )
    met_loss = loss_near + shifted(loss_far, "core", 1)
    met_dunit = part_near + shifted(part_far, "core", 1)
    met_low = met.astype(jnp.float32)
    along = jnp.sum(met_low * met_dunit, axis=1)
    across = (met_dunit - met_low * along[:, None]).astype(jnp.float16)
    home = shifted_by_window(with_rows(across, *digits(along), *digits(met_loss)), window, 1)
    txt_unit, txt_len = unit_rows(lax.dynamic_slice_in_dim(txt_emb, z * rows, rows, 0))
    text_low = txt_unit.astype(jnp.bfloat16)
    text_other = shifted(text_low, "core", 1)
    own_index = place * rows + lax.iota(jnp.int32, rows)
    other_place = place + jnp.where(core == 0, z_size, -z_size)
    other_index = other_place * rows + lax.iota(jnp.int32, rows)

    def text_side(texts, text_index, blocks):
        columns = jnp.concatenate([piece[:rows] for piece in blocks])
        positive = is_match(text_index.astype(jnp.float32), matches(blocks))
        coef = coefs(logits(texts, columns, scale, shift_value), positive, scale)
        return jnp.dot(coef, columns, preferred_element_type=jnp.float32)

    here[4], after[4], home = lax.optimization_barrier((here[4], after[4], home))
    home = home.astype(jnp.float32)
    tail = home[rows]
    along = tail[:rows] + tail[rows : 2 * rows] * (1.0 / LOW_SCALE)
    row_loss = tail[2 * rows : 3 * rows] + tail[3 * rows : 4 * rows] * (1.0 / LOW_SCALE)
    image_dunit = home[:rows] + image_low.astype(jnp.float32) * along[:, None]
    img_grad = (
        image_dunit - img_unit * jnp.sum(img_unit * image_dunit, axis=1, keepdims=True)
    ) / img_len

    near_part = far_part = 0.0
    for group in ((0, 1, -1, 2, -2), (3, -3, 4)):
        near = [jnp.where((z - d) % z_size >= z, here[d], after[d]) for d in group]
        far = [jnp.where(core == 0, after[d], here[d]) for d in group]
        near_part = near_part + text_side(text_low, own_index, near)
        far_part = far_part + text_side(text_other, other_index, far)
    text_dunit = near_part + shifted(far_part, "core", 1)
    txt_grad = (
        text_dunit - txt_unit * jnp.sum(txt_unit * text_dunit, axis=1, keepdims=True)
    ) / txt_len
    return (img_grad, txt_grad, row_loss)


def solution(mesh):
    z_size = mesh.shape["tensor"]
    fine = Mesh(mesh.devices.reshape(-1, 2, z_size), ALL)
    in_specs = (
        P(ROWS_OF, "z"),
        P("z", None),
        P(ALL, None),
        P(ROWS_OF, "z"),
        P("z", None),
        P(),
        P(),
        P(ALL),
        P(),
    )
    out_specs = (P(ALL, None), P(ALL, None), P(ALL))
    return jax.shard_map(body, mesh=fine, in_specs=in_specs, out_specs=out_specs, check_vma=False)
```

```python
import jax
import jax.numpy as jnp
from jax import lax
from jax.sharding import Mesh, PartitionSpec as P

SUM_SCALE = 1024.0
LOW_SCALE = 2048.0
EXTRA = 8
LANES = 128
ROWS_OF = ("chip", "core")
ALL = ("chip", "core", "z")


def shifted(shard, axis, by):
    devices = lax.axis_size(axis)
    return lax.ppermute(shard, axis, [(i, (i + by) % devices) for i in range(devices)])


def shifted_by_window(shard, window, sign):
    chips = lax.axis_size("chip")

    def branch(by):
        if by == 0:
            return lambda value: value
        return lambda value: shifted(value, "chip", sign * by)

    return lax.switch(window, [branch(by) for by in range(chips)], shard)


def with_rows(block, *vectors):
    row = jnp.concatenate(vectors)[None, :].astype(block.dtype)
    return jnp.concatenate(
        [block, jnp.pad(row, ((0, EXTRA - 1), (0, block.shape[1] - row.shape[1])))]
    )


def ring_gather(block):
    up = down = block
    found = [block]
    for _ in range(3):
        up = shifted(up, "z", 1)
        down = shifted(down, "z", -1)
        found += [up, down]
    return [*found, shifted(down, "z", -1)]


def ring_sum(parts, z):
    size = parts.shape[0]

    def mine(ahead):
        return lax.dynamic_index_in_dim(parts, (z + ahead) % size, 0, False)

    def sent(up, down):
        up = shifted(up.astype(jnp.float16), "z", 1)
        down = shifted(down.astype(jnp.float16), "z", -1)
        up, down = lax.optimization_barrier((up, down))
        return up.astype(jnp.float32), down.astype(jnp.float32)

    up, down = mine(size // 2), mine(1 - size // 2)
    for ahead in range(size // 2 - 1, 0, -1):
        up, down = sent(up, down)
        up, down = mine(ahead) + up, mine(1 - ahead) + down
    return down + shifted(up.astype(jnp.float16), "z", 1).astype(jnp.float32)


def digits(value):
    high = value.astype(jnp.float16)
    return high, ((value - high.astype(jnp.float32)) * LOW_SCALE).astype(jnp.float16)


def unit_rows(emb):
    length = jnp.sqrt(jnp.sum(emb * emb, axis=1, keepdims=True) + 1e-06)
    return (emb / length, length)


def logits(rows, columns, scale, shift_value):
    cosine = lax.dot_general(
        rows, columns, (((1,), (1,)), ((), ())), preferred_element_type=jnp.float32
    )
    return scale * cosine + shift_value


def coefs(logit, positive, scale):
    return ((jax.nn.sigmoid(logit) - positive.astype(jnp.float32)) * scale).astype(jnp.bfloat16)


def body(
    img_hidden, img_down, img_pooled, txt_hidden, txt_proj, log_temp, bias, match, window_index
):
    rows, width = img_pooled.shape
    scale = jnp.exp(log_temp[0])
    shift_value = bias[0]
    window = window_index[0]
    place = lax.axis_index(ALL)
    devices = lax.axis_size(ALL)
    z = lax.axis_index("z")
    z_size = lax.axis_size("z")
    core = lax.axis_index("core")
    column = z_size * rows
    total_rows = devices * rows

    img_part = jnp.dot(img_hidden, img_down, preferred_element_type=jnp.float32) * SUM_SCALE
    img_sum = ring_sum(img_part.reshape(z_size, rows, width), z) * (1.0 / SUM_SCALE)

    share = (width + LANES) // 2
    proj_part = jnp.where(core == 0, txt_proj[:, :share], txt_proj[:, width - share :])
    pieces = ring_gather(jnp.concatenate([txt_hidden.T, proj_part], axis=1))
    parts = (pieces[:3], pieces[3:5], pieces[5:])
    here_parts = [jnp.concatenate([piece[:, :column] for piece in part]) for part in parts]
    before_parts = [shifted(here_parts[0], "chip", 1), shifted(here_parts[1], "chip", 1)]
    proj_mine = jnp.concatenate([piece[:, column:] for piece in pieces])
    proj_other = shifted(proj_mine, "core", 1)
    proj = jnp.concatenate(
        [
            jnp.where(core == 0, proj_mine, proj_other),
            jnp.where(core == 0, proj_other, proj_mine)[:, 2 * share - width :],
        ],
        axis=1,
    )
    def text_head(hidden_parts):
        emb, row = 0.0, 0
        for hidden in hidden_parts:
            emb = emb + lax.dot_general(
                hidden,
                proj[row : row + hidden.shape[0]],
                (((0,), (0,)), ((), ())),
                preferred_element_type=jnp.float32,
            )
            row += hidden.shape[0]
        return emb

    img_emb = img_sum + img_pooled.astype(jnp.float32)
    img_unit, img_len = unit_rows(img_emb)
    image_low = img_unit.astype(jnp.bfloat16)
    block = with_rows(image_low, match // rows, match % rows)
    block = shifted_by_window(block, window, -1)
    block, here_parts[2] = lax.optimization_barrier((block, here_parts[2]))
    before_parts.append(shifted(here_parts[2], "chip", 1))
    txt_emb = text_head(here_parts)
    text_here = unit_rows(txt_emb)[0].astype(jnp.bfloat16)
    text_before = unit_rows(text_head(before_parts))[0].astype(jnp.bfloat16)
    txt_unit, txt_len = unit_rows(lax.dynamic_slice_in_dim(txt_emb, z * rows, rows, 0))
    text_low = txt_unit.astype(jnp.bfloat16)
    texts = jnp.concatenate([text_low, shifted(text_low, "core", 1)])

    block_other = shifted(block, "core", 1)

    after_0 = shifted(block, "chip", -1)
    up = jnp.stack([shifted(block, "z", 1), after_0])
    down = jnp.stack([shifted(block, "z", -1), after_0])
    landed = [(block[None], ((0, True),)), (up, ((1, True), (0, False))), (down[:1], ((-1, True),))]
    for step in (2, 3, 4):
        up = shifted(up, "z", 1)
        if step < 4:
            down = shifted(down, "z", -1)
            landed.append((down, ((-step, True), (1 - step, False))))
        if step == 2:
            up, text_here = lax.optimization_barrier((up, text_here))
        if step == 3:
            up, text_before = lax.optimization_barrier((up, text_before))
        landed.append((up, ((step, True), (step - 1, False))))
    after_3 = shifted(down[1], "z", -1)
    after_4 = shifted(after_3, "z", -1)
    landed.append((after_3[None], ((-3, False),)))
    last = after_4[None], ((4, False),)

    row_iota = lax.iota(jnp.int32, column)
    block_of = row_iota // rows
    column_base = (place - z) * rows

    is_here = block_of <= z
    text_near = jnp.where(is_here[:, None], text_here, text_before)
    near_index = column_base + row_iota - jnp.where(is_here, 0, 2 * column)
    near_index = near_index % total_rows
    text_far = jnp.where(core == 0, text_here, text_before)
    far_index = column_base + row_iota - jnp.where(core == 0, 0, 2 * column)
    far_index = far_index % total_rows

    def matches(blocks):
        found = [piece[rows].astype(jnp.float32) for piece in blocks]
        return jnp.concatenate([row[:rows] * rows + row[rows : 2 * rows] for row in found])

    def is_match(row_values, column_values):
        return row_values[:, None] == column_values.astype(jnp.float32)[None, :]

    def image_side(images, image_match, columns, index):
        positive = is_match(image_match, index)
        logit = logits(images, columns, scale, shift_value)
        loss = jnp.sum(
            jnp.where(positive, jax.nn.softplus(-logit), jax.nn.softplus(logit)), axis=1
        )
        coef = coefs(logit, positive, scale)
        return loss, jnp.dot(coef, columns, preferred_element_type=jnp.float32)

    met = block[:rows]
    loss_near, part_near = image_side(met, matches([block]), text_near, near_index)
    loss_far, part_far = image_side(
        block_other[:rows], matches([block_other]), text_far, far_index
    )
    met_loss = loss_near + shifted(loss_far, "core", 1)
    met_dunit = part_near + shifted(part_far, "core", 1)
    met_low = met.astype(jnp.float32)
    along = jnp.sum(met_low * met_dunit, axis=1)
    across = (met_dunit - met_low * along[:, None]).astype(jnp.float16)
    home = shifted_by_window(with_rows(across, *digits(along), *digits(met_loss)), window, 1)
    other_place = place + jnp.where(core == 0, z_size, -z_size)
    text_index = jnp.concatenate([place * rows + row_iota[:rows], other_place * rows + row_iota[:rows]])
    is_own = lax.iota(jnp.int32, 2 * rows) < rows
    block_rows = rows + EXTRA
    is_row = lax.iota(jnp.int32, block_rows) < rows

    def text_side(stack, kinds):
        columns = stack.reshape(-1, width)
        image_match, is_used = [], []
        for i, (distance, is_here_block) in enumerate(kinds):
            image_match.append(jnp.pad(matches([stack[i]]), (0, EXTRA)))
            in_near = ((z - distance) % z_size >= z) == is_here_block
            in_far = (core == 1) == is_here_block
            is_used.append(jnp.where(is_own, in_near, in_far)[:, None] & is_row[None, :])
        logit = logits(texts, columns, scale, shift_value)
        positive = is_match(text_index.astype(jnp.float32), jnp.concatenate(image_match))
        coef = coefs(logit, positive, scale)
        coef = jnp.where(jnp.concatenate(is_used, axis=1), coef, jnp.bfloat16(0))
        return jnp.dot(coef, columns, preferred_element_type=jnp.float32)

    pair_dunit = sum(text_side(*item) for item in landed)
    pair_dunit, home, met = lax.optimization_barrier((pair_dunit, home, last[0]))
    home = home.astype(jnp.float32)
    tail = home[rows]
    along = tail[:rows] + tail[rows : 2 * rows] * (1.0 / LOW_SCALE)
    row_loss = tail[2 * rows : 3 * rows] + tail[3 * rows : 4 * rows] * (1.0 / LOW_SCALE)
    image_dunit = home[:rows] + image_low.astype(jnp.float32) * along[:, None]
    img_grad = (
        image_dunit - img_unit * jnp.sum(img_unit * image_dunit, axis=1, keepdims=True)
    ) / img_len

    pair_dunit = pair_dunit + text_side(met, last[1])
    text_dunit = pair_dunit[:rows] + shifted(pair_dunit[rows:], "core", 1)
    txt_grad = (
        text_dunit - txt_unit * jnp.sum(txt_unit * text_dunit, axis=1, keepdims=True)
    ) / txt_len
    return (img_grad, txt_grad, row_loss)


def solution(mesh):
    z_size = mesh.shape["tensor"]
    fine = Mesh(mesh.devices.reshape(-1, 2, z_size), ALL)
    in_specs = (
        P(ROWS_OF, "z"),
        P("z", None),
        P(ALL, None),
        P(ROWS_OF, "z"),
        P("z", None),
        P(),
        P(),
        P(ALL),
        P(),
    )
    out_specs = (P(ALL, None), P(ALL, None), P(ALL))
    return jax.shard_map(body, mesh=fine, in_specs=in_specs, out_specs=out_specs, check_vma=False)
```

```python
import jax
import jax.numpy as jnp
from jax import lax
from jax.experimental import pallas as pl
from jax.experimental.pallas import tpu as pltpu
from jax.sharding import Mesh, PartitionSpec as P

SUM_SCALE = 1024.0
LOW_SCALE = 2048.0
EXTRA = 8
LANES = 128
ROWS_OF = ("chip", "core")
ALL = ("chip", "core", "z")


def shifted(shard, axis, by):
    devices = lax.axis_size(axis)
    return lax.ppermute(shard, axis, [(i, (i + by) % devices) for i in range(devices)])


def shifted_by_window(shard, window, sign):
    chips = lax.axis_size("chip")

    def branch(by):
        if by == 0:
            return lambda value: value
        return lambda value: shifted(value, "chip", sign * by)

    return lax.switch(window, [branch(by) for by in range(chips)], shard)


def with_rows(block, *vectors):
    row = jnp.concatenate(vectors)[None, :].astype(block.dtype)
    return jnp.concatenate(
        [block, jnp.pad(row, ((0, EXTRA - 1), (0, block.shape[1] - row.shape[1])))]
    )


def ring_gather(block):
    up = down = block
    found = [block]
    for _ in range(3):
        up = shifted(up, "z", 1)
        down = shifted(down, "z", -1)
        found += [up, down]
    return [*found, shifted(down, "z", -1)]


def ring_sum(parts, z):
    size = parts.shape[0]

    def mine(ahead):
        return lax.dynamic_index_in_dim(parts, (z + ahead) % size, 0, False)

    def sent(up, down):
        up = shifted(up.astype(jnp.float16), "z", 1)
        down = shifted(down.astype(jnp.float16), "z", -1)
        up, down = lax.optimization_barrier((up, down))
        return up.astype(jnp.float32), down.astype(jnp.float32)

    up, down = mine(size // 2), mine(1 - size // 2)
    for ahead in range(size // 2 - 1, 0, -1):
        up, down = sent(up, down)
        up, down = mine(ahead) + up, mine(1 - ahead) + down
    return down + shifted(up.astype(jnp.float16), "z", 1).astype(jnp.float32)


def digits(value):
    high = value.astype(jnp.float16)
    return high, ((value - high.astype(jnp.float32)) * LOW_SCALE).astype(jnp.float16)


def unit_rows(emb):
    length = jnp.sqrt(jnp.sum(emb * emb, axis=1, keepdims=True) + 1e-06)
    return (emb / length, length)


def tile_logits(rows, columns, scale, shift_value):
    cosine = lax.dot_general(
        rows, columns, (((1,), (1,)), ((), ())), preferred_element_type=jnp.float32
    )
    return scale * cosine + shift_value


def used_rows(near, far, rows, count):
    is_near = lax.broadcasted_iota(jnp.int32, (count, 1), 0) < rows
    return jnp.where(is_near, near, far) > 0


def text_tiles(texts, text_index, numbers, uses, stacks, kinds):
    count, width = texts.shape
    rows = count // 2

    def kernel(numbers_ref, uses_ref, texts_ref, index_ref, *refs):
        stack_refs, out_ref = refs[:-1], refs[-1]
        scale, shift_value = numbers_ref[0], numbers_ref[1]
        texts_now, index = texts_ref[...], index_ref[...]
        total = jnp.zeros((count, width), jnp.float32)
        for first in range(0, len(kinds), 2):
            columns, match, used = [], [], []
            for at in range(first, min(first + 2, len(kinds))):
                which, i = kinds[at]
                block = stack_refs[which]
                columns.append(block[i, :rows, :])
                digit = block[i, rows : rows + EXTRA, : 2 * rows].astype(jnp.float32)
                match.append(digit[:1, :rows] * rows + digit[:1, rows:])
                near, far = uses_ref[2 * at], uses_ref[2 * at + 1]
                used.append(jnp.broadcast_to(used_rows(near, far, rows, count), (count, rows)))
            columns = jnp.concatenate(columns, axis=0)
            logit = tile_logits(texts_now, columns, scale, shift_value)
            positive = index == jnp.concatenate(match, axis=1)
            coef = (jax.nn.sigmoid(logit) - positive.astype(jnp.float32)) * scale
            coef = jnp.where(jnp.concatenate(used, axis=1), coef, 0.0).astype(jnp.bfloat16)
            total = total + jnp.dot(coef, columns, preferred_element_type=jnp.float32)
        out_ref[...] = total

    work = 4 * count * rows * width * len(kinds)
    return pl.pallas_call(
        kernel,
        out_shape=jax.ShapeDtypeStruct((count, width), jnp.float32),
        in_specs=[pl.BlockSpec(memory_space=pltpu.SMEM)] * 2
        + [pl.BlockSpec(memory_space=pltpu.VMEM)] * (2 + len(stacks)),
        out_specs=pl.BlockSpec(memory_space=pltpu.VMEM),
        cost_estimate=pl.CostEstimate(flops=work, bytes_accessed=0, transcendentals=0),
        name="text_tiles",
    )(numbers, uses, texts, text_index, *stacks)


def image_tiles(images, image_match, numbers, uses, bases, text_here, text_before):
    count, width = images.shape
    rows = count // 2
    blocks = text_here.shape[0] // rows

    def kernel(
        numbers_ref, uses_ref, bases_ref, images_ref, match_ref, here_ref, before_ref, out_ref,
        loss_ref,
    ):
        scale, shift_value = numbers_ref[0], numbers_ref[1]
        images_now, match = images_ref[...], match_ref[...]
        total = jnp.zeros((count, width), jnp.float32)
        loss = jnp.zeros((count, 2 * rows), jnp.float32)
        lane = lax.broadcasted_iota(jnp.int32, (1, rows), 1)
        for at in range(blocks):
            span = pl.ds(at * rows, rows)
            columns = jnp.concatenate([here_ref[span, :], before_ref[span, :]], axis=0)
            index = jnp.concatenate([lane + (bases_ref[i] + at * rows) for i in range(2)], axis=1)
            used = [
                jnp.broadcast_to(
                    used_rows(uses_ref[4 * at + 2 * i], uses_ref[4 * at + 2 * i + 1], rows, count),
                    (count, rows),
                )
                for i in range(2)
            ]
            used = jnp.concatenate(used, axis=1)
            logit = tile_logits(images_now, columns, scale, shift_value)
            positive = match == index
            signed = jnp.where(positive, -logit, logit)
            pair_loss = jnp.maximum(signed, 0.0) + jnp.log1p(jnp.exp(-jnp.abs(signed)))
            loss = loss + jnp.where(used, pair_loss, 0.0)
            coef = (jax.nn.sigmoid(logit) - positive.astype(jnp.float32)) * scale
            coef = jnp.where(used, coef, 0.0).astype(jnp.bfloat16)
            total = total + jnp.dot(coef, columns, preferred_element_type=jnp.float32)
        out_ref[...] = total
        loss_ref[...] = jnp.broadcast_to(jnp.sum(loss, axis=1, keepdims=True), (count, LANES))

    work = 8 * count * rows * width * blocks
    return pl.pallas_call(
        kernel,
        out_shape=(
            jax.ShapeDtypeStruct((count, width), jnp.float32),
            jax.ShapeDtypeStruct((count, LANES), jnp.float32),
        ),
        in_specs=[pl.BlockSpec(memory_space=pltpu.SMEM)] * 3
        + [pl.BlockSpec(memory_space=pltpu.VMEM)] * 4,
        out_specs=[pl.BlockSpec(memory_space=pltpu.VMEM)] * 2,
        cost_estimate=pl.CostEstimate(flops=work, bytes_accessed=0, transcendentals=0),
        name="image_tiles",
    )(numbers, uses, bases, images, image_match, text_here, text_before)


def body(
    img_hidden, img_down, img_pooled, txt_hidden, txt_proj, log_temp, bias, match, window_index
):
    rows, width = img_pooled.shape
    scale = jnp.exp(log_temp[0])
    shift_value = bias[0]
    window = window_index[0]
    place = lax.axis_index(ALL)
    devices = lax.axis_size(ALL)
    z = lax.axis_index("z")
    z_size = lax.axis_size("z")
    core = lax.axis_index("core")
    column = z_size * rows
    total_rows = devices * rows

    img_part = jnp.dot(img_hidden, img_down, preferred_element_type=jnp.float32) * SUM_SCALE
    img_sum = ring_sum(img_part.reshape(z_size, rows, width), z) * (1.0 / SUM_SCALE)

    share = (width + LANES) // 2
    proj_part = jnp.where(core == 0, txt_proj[:, :share], txt_proj[:, width - share :])
    pieces = ring_gather(jnp.concatenate([txt_hidden.T, proj_part], axis=1))
    parts = (pieces[:3], pieces[3:5], pieces[5:])
    here_parts = [jnp.concatenate([piece[:, :column] for piece in part]) for part in parts]
    before_parts = [shifted(here_parts[0], "chip", 1), shifted(here_parts[1], "chip", 1)]
    proj_mine = jnp.concatenate([piece[:, column:] for piece in pieces])
    proj_other = shifted(proj_mine, "core", 1)
    proj = jnp.concatenate(
        [
            jnp.where(core == 0, proj_mine, proj_other),
            jnp.where(core == 0, proj_other, proj_mine)[:, 2 * share - width :],
        ],
        axis=1,
    )
    def text_head(hidden_parts):
        emb, row = 0.0, 0
        for hidden in hidden_parts:
            emb = emb + lax.dot_general(
                hidden,
                proj[row : row + hidden.shape[0]],
                (((0,), (0,)), ((), ())),
                preferred_element_type=jnp.float32,
            )
            row += hidden.shape[0]
        return emb

    img_emb = img_sum + img_pooled.astype(jnp.float32)
    img_unit, img_len = unit_rows(img_emb)
    image_low = img_unit.astype(jnp.bfloat16)
    block = with_rows(image_low, match // rows, match % rows)
    block = shifted_by_window(block, window, -1)
    block, here_parts[2] = lax.optimization_barrier((block, here_parts[2]))
    before_parts.append(shifted(here_parts[2], "chip", 1))
    txt_emb = text_head(here_parts)
    text_here = unit_rows(txt_emb)[0].astype(jnp.bfloat16)
    text_before = unit_rows(text_head(before_parts))[0].astype(jnp.bfloat16)
    txt_unit, txt_len = unit_rows(lax.dynamic_slice_in_dim(txt_emb, z * rows, rows, 0))
    text_low = txt_unit.astype(jnp.bfloat16)
    texts = jnp.concatenate([text_low, shifted(text_low, "core", 1)])

    block_other = shifted(block, "core", 1)

    after_0 = shifted(block, "chip", -1)
    up = jnp.stack([shifted(block, "z", 1), after_0])
    down = jnp.stack([shifted(block, "z", -1), after_0])
    landed = [(block[None], ((0, True),)), (up, ((1, True), (0, False))), (down, ((-1, True),))]
    for step in (2, 3):
        up, down = shifted(up, "z", 1), shifted(down, "z", -1)
        if step == 2:
            up, text_here = lax.optimization_barrier((up, text_here))
        else:
            up, text_before = lax.optimization_barrier((up, text_before))
        landed.append((up, ((step, True), (step - 1, False))))
        landed.append((down, ((-step, True), (1 - step, False))))
    up = shifted(up, "z", 1)
    after_3 = shifted(down[1], "z", -1)
    after_4 = shifted(after_3, "z", -1)
    last = [(up, ((4, True), (3, False))), (after_3[None], ((-3, False),))]
    last.append((after_4[None], ((4, False),)))

    column_base = (place - z) * rows
    numbers = jnp.stack([scale, shift_value])
    blocks_of = jnp.arange(z_size, dtype=jnp.int32)
    near_here = blocks_of <= z
    far_here = jnp.full((z_size,), core == 0)
    image_uses = jnp.stack([near_here, far_here, ~near_here, ~far_here], axis=1)
    bases = jnp.stack([column_base, (column_base - 2 * column) % total_rows])

    def matches(piece):
        row = piece[rows].astype(jnp.int32)
        return row[:rows] * rows + row[rows : 2 * rows]

    met = block[:rows]
    met_dunit, met_loss = image_tiles(
        jnp.concatenate([met, block_other[:rows]]),
        jnp.concatenate([matches(block), matches(block_other)])[:, None],
        numbers,
        image_uses.astype(jnp.int32).reshape(-1),
        bases,
        text_here,
        text_before,
    )
    met_loss = met_loss[:rows, 0] + shifted(met_loss[rows:, 0], "core", 1)
    met_dunit = met_dunit[:rows] + shifted(met_dunit[rows:], "core", 1)
    met_low = met.astype(jnp.float32)
    along = jnp.sum(met_low * met_dunit, axis=1)
    across = (met_dunit - met_low * along[:, None]).astype(jnp.float16)
    home = shifted_by_window(with_rows(across, *digits(along), *digits(met_loss)), window, 1)
    row_iota = lax.iota(jnp.int32, rows)
    other_place = place + jnp.where(core == 0, z_size, -z_size)
    text_index = jnp.concatenate([place * rows + row_iota, other_place * rows + row_iota])
    text_index = text_index.astype(jnp.float32)[:, None]

    def text_side(group):
        kinds, uses = [], []
        for which, (_, blocks) in enumerate(group):
            for i, (distance, is_here) in enumerate(blocks):
                kinds.append((which, i))
                uses += [((z - distance) % z_size >= z) == is_here, (core == 1) == is_here]
        uses = jnp.stack(uses).astype(jnp.int32)
        return text_tiles(texts, text_index, numbers, uses, [item[0] for item in group], kinds)

    early_dunit = text_side(landed)
    early_dunit, home, last_up = lax.optimization_barrier((early_dunit, home, last[0][0]))
    last[0] = (last_up, last[0][1])
    pair_dunit = early_dunit + text_side(last)
    home = home.astype(jnp.float32)
    tail = home[rows]
    along = tail[:rows] + tail[rows : 2 * rows] * (1.0 / LOW_SCALE)
    row_loss = tail[2 * rows : 3 * rows] + tail[3 * rows : 4 * rows] * (1.0 / LOW_SCALE)
    image_dunit = home[:rows] + image_low.astype(jnp.float32) * along[:, None]
    img_grad = (
        image_dunit - img_unit * jnp.sum(img_unit * image_dunit, axis=1, keepdims=True)
    ) / img_len

    text_dunit = pair_dunit[:rows] + shifted(pair_dunit[rows:], "core", 1)
    txt_grad = (
        text_dunit - txt_unit * jnp.sum(txt_unit * text_dunit, axis=1, keepdims=True)
    ) / txt_len
    return (img_grad, txt_grad, row_loss)


def solution(mesh):
    z_size = mesh.shape["tensor"]
    fine = Mesh(mesh.devices.reshape(-1, 2, z_size), ALL)
    in_specs = (
        P(ROWS_OF, "z"),
        P("z", None),
        P(ALL, None),
        P(ROWS_OF, "z"),
        P("z", None),
        P(),
        P(),
        P(ALL),
        P(),
    )
    out_specs = (P(ALL, None), P(ALL, None), P(ALL))
    return jax.shard_map(body, mesh=fine, in_specs=in_specs, out_specs=out_specs, check_vma=False)
```

```python
import jax
import jax.numpy as jnp
from jax import lax
from jax.experimental import pallas as pl
from jax.experimental.pallas import tpu as pltpu
from jax.sharding import Mesh, PartitionSpec as P


SUM_SCALE = 1024.0
LOW_SCALE = 2048.0
EXTRA = 8
LANES = 128
ROWS_OF = ("chip", "core")
ALL = ("chip", "core", "z")


def shifted(shard, axis, by):
    devices = lax.axis_size(axis)
    return lax.ppermute(shard, axis, [(i, (i + by) % devices) for i in range(devices)])


def step_of_ring(shard, by):
    return shifted(shard, "z", by)


def shifted_by_window(shard, window, sign):
    chips = lax.axis_size("chip")

    def branch(by):
        if by == 0:
            return lambda value: value
        return lambda value: shifted(value, "chip", sign * by)

    return lax.switch(window, [branch(by) for by in range(chips)], shard)


def with_rows(block, *vectors):
    row = jnp.concatenate(vectors)[None, :].astype(block.dtype)
    return jnp.concatenate(
        [block, jnp.pad(row, ((0, EXTRA - 1), (0, block.shape[1] - row.shape[1])))]
    )


def ring_gather(block):
    up = down = block
    found = [block]
    for _ in range(3):
        up = shifted(up, "z", 1)
        down = shifted(down, "z", -1)
        found += [up, down]
    return [*found, shifted(down, "z", -1)]


def ring_sum(parts, z):
    size = parts.shape[0]

    def mine(ahead):
        return lax.dynamic_index_in_dim(parts, (z + ahead) % size, 0, False)

    def sent(up, down):
        up = shifted(up.astype(jnp.float16), "z", 1)
        down = shifted(down.astype(jnp.float16), "z", -1)
        up, down = lax.optimization_barrier((up, down))
        return up.astype(jnp.float32), down.astype(jnp.float32)

    up, down = mine(size // 2), mine(1 - size // 2)
    for ahead in range(size // 2 - 1, 0, -1):
        up, down = sent(up, down)
        up, down = mine(ahead) + up, mine(1 - ahead) + down
    return down + shifted(up.astype(jnp.float16), "z", 1).astype(jnp.float32)


def digits(value):
    high = value.astype(jnp.float16)
    return high, ((value - high.astype(jnp.float32)) * LOW_SCALE).astype(jnp.float16)


def unit_rows(emb):
    length = jnp.sqrt(jnp.sum(emb * emb, axis=1, keepdims=True) + 1e-06)
    return (emb / length, length)


def tile_logits(rows, columns, scale, shift_value):
    cosine = lax.dot_general(
        rows, columns, (((1,), (1,)), ((), ())), preferred_element_type=jnp.float32
    )
    return scale * cosine + shift_value


def used_rows(near, far, rows, count):
    is_near = lax.broadcasted_iota(jnp.int32, (count, 1), 0) < rows
    return jnp.where(is_near, near, far) > 0


def text_tiles(texts, text_index, numbers, uses, stacks, kinds):
    count, width = texts.shape
    rows = count // 2

    def kernel(numbers_ref, uses_ref, texts_ref, index_ref, *refs):
        stack_refs, out_ref = refs[:-1], refs[-1]
        scale, shift_value = numbers_ref[0], numbers_ref[1]
        texts_now, index = texts_ref[...], index_ref[...]
        total = jnp.zeros((count, width), jnp.float32)
        for first in range(0, len(kinds), 2):
            columns, match, used = [], [], []
            for at in range(first, min(first + 2, len(kinds))):
                which, i = kinds[at]
                block = stack_refs[which]
                columns.append(block[i, :rows, :])
                digit = block[i, rows : rows + EXTRA, : 2 * rows].astype(jnp.float32)
                match.append(digit[:1, :rows] * rows + digit[:1, rows:])
                near, far = uses_ref[2 * at], uses_ref[2 * at + 1]
                used.append(jnp.broadcast_to(used_rows(near, far, rows, count), (count, rows)))
            columns = jnp.concatenate(columns, axis=0)
            logit = tile_logits(texts_now, columns, scale, shift_value)
            positive = index == jnp.concatenate(match, axis=1)
            coef = (jax.nn.sigmoid(logit) - positive.astype(jnp.float32)) * scale
            coef = jnp.where(jnp.concatenate(used, axis=1), coef, 0.0).astype(jnp.bfloat16)
            total = total + jnp.dot(coef, columns, preferred_element_type=jnp.float32)
        out_ref[...] = total

    work = 4 * count * rows * width * len(kinds)
    return pl.pallas_call(
        kernel,
        out_shape=jax.ShapeDtypeStruct((count, width), jnp.float32),
        in_specs=[pl.BlockSpec(memory_space=pltpu.SMEM)] * 2
        + [pl.BlockSpec(memory_space=pltpu.VMEM)] * (2 + len(stacks)),
        out_specs=pl.BlockSpec(memory_space=pltpu.VMEM),
        cost_estimate=pl.CostEstimate(flops=work, bytes_accessed=0, transcendentals=0),
        name="text_tiles",
    )(numbers, uses, texts, text_index, *stacks)


def image_tiles(images, image_match, numbers, uses, bases, text_here, text_before):
    count, width = images.shape
    rows = count // 2
    blocks = text_here.shape[0] // rows

    def kernel(
        numbers_ref, uses_ref, bases_ref, images_ref, match_ref, here_ref, before_ref, out_ref,
        loss_ref,
    ):
        scale, shift_value = numbers_ref[0], numbers_ref[1]
        images_now, match = images_ref[...], match_ref[...]
        total = jnp.zeros((count, width), jnp.float32)
        loss = jnp.zeros((count, 2 * rows), jnp.float32)
        lane = lax.broadcasted_iota(jnp.int32, (1, rows), 1)
        for at in range(blocks):
            span = pl.ds(at * rows, rows)
            columns = jnp.concatenate([here_ref[span, :], before_ref[span, :]], axis=0)
            index = jnp.concatenate([lane + (bases_ref[i] + at * rows) for i in range(2)], axis=1)
            used = [
                jnp.broadcast_to(
                    used_rows(uses_ref[4 * at + 2 * i], uses_ref[4 * at + 2 * i + 1], rows, count),
                    (count, rows),
                )
                for i in range(2)
            ]
            used = jnp.concatenate(used, axis=1)
            logit = tile_logits(images_now, columns, scale, shift_value)
            positive = match == index
            signed = jnp.where(positive, -logit, logit)
            pair_loss = jnp.maximum(signed, 0.0) + jnp.log1p(jnp.exp(-jnp.abs(signed)))
            loss = loss + jnp.where(used, pair_loss, 0.0)
            coef = (jax.nn.sigmoid(logit) - positive.astype(jnp.float32)) * scale
            coef = jnp.where(used, coef, 0.0).astype(jnp.bfloat16)
            total = total + jnp.dot(coef, columns, preferred_element_type=jnp.float32)
        out_ref[...] = total
        loss_ref[...] = jnp.broadcast_to(jnp.sum(loss, axis=1, keepdims=True), (count, LANES))

    work = 8 * count * rows * width * blocks
    return pl.pallas_call(
        kernel,
        out_shape=(
            jax.ShapeDtypeStruct((count, width), jnp.float32),
            jax.ShapeDtypeStruct((count, LANES), jnp.float32),
        ),
        in_specs=[pl.BlockSpec(memory_space=pltpu.SMEM)] * 3
        + [pl.BlockSpec(memory_space=pltpu.VMEM)] * 4,
        out_specs=[pl.BlockSpec(memory_space=pltpu.VMEM)] * 2,
        cost_estimate=pl.CostEstimate(flops=work, bytes_accessed=0, transcendentals=0),
        name="image_tiles",
    )(numbers, uses, bases, images, image_match, text_here, text_before)


def body(
    img_hidden, img_down, img_pooled, txt_hidden, txt_proj, log_temp, bias, match, window_index
):
    rows, width = img_pooled.shape
    scale = jnp.exp(log_temp[0])
    shift_value = bias[0]
    window = window_index[0]
    place = lax.axis_index(ALL)
    devices = lax.axis_size(ALL)
    z = lax.axis_index("z")
    z_size = lax.axis_size("z")
    core = lax.axis_index("core")
    column = z_size * rows
    total_rows = devices * rows

    img_part = jnp.dot(img_hidden, img_down, preferred_element_type=jnp.float32) * SUM_SCALE
    img_sum = ring_sum(img_part.reshape(z_size, rows, width), z) * (1.0 / SUM_SCALE)

    share = (width + LANES) // 2
    proj_part = jnp.where(core == 0, txt_proj[:, :share], txt_proj[:, width - share :])
    pieces = ring_gather(jnp.concatenate([txt_hidden.T, proj_part], axis=1))
    parts = (pieces[:3], pieces[3:5], pieces[5:])
    here_parts = [jnp.concatenate([piece[:, :column] for piece in part]) for part in parts]
    before_parts = [shifted(here_parts[0], "chip", 1), shifted(here_parts[1], "chip", 1)]
    proj_mine = jnp.concatenate([piece[:, column:] for piece in pieces])
    proj_other = shifted(proj_mine, "core", 1)
    proj = jnp.concatenate(
        [
            jnp.where(core == 0, proj_mine, proj_other),
            jnp.where(core == 0, proj_other, proj_mine)[:, 2 * share - width :],
        ],
        axis=1,
    )

    def text_head(hidden_parts):
        emb, row = 0.0, 0
        for hidden in hidden_parts:
            emb = emb + lax.dot_general(
                hidden,
                proj[row : row + hidden.shape[0]],
                (((0,), (0,)), ((), ())),
                preferred_element_type=jnp.float32,
            )
            row += hidden.shape[0]
        return emb

    img_emb = img_sum + img_pooled.astype(jnp.float32)
    img_unit, img_len = unit_rows(img_emb)
    image_low = img_unit.astype(jnp.bfloat16)
    block = with_rows(image_low, match // rows, match % rows)
    block = shifted_by_window(block, window, -1)
    block, here_parts[2] = lax.optimization_barrier((block, here_parts[2]))
    before_parts.append(shifted(here_parts[2], "chip", 1))
    txt_emb = text_head(here_parts)
    text_here = unit_rows(txt_emb)[0].astype(jnp.bfloat16)
    text_before = unit_rows(text_head(before_parts))[0].astype(jnp.bfloat16)
    txt_unit, txt_len = unit_rows(lax.dynamic_slice_in_dim(txt_emb, z * rows, rows, 0))
    text_low = txt_unit.astype(jnp.bfloat16)
    texts = jnp.concatenate([text_low, shifted(text_low, "core", 1)])

    block_other = shifted(block, "core", 1)

    after_0 = shifted(block, "chip", -1)
    up = jnp.stack([shifted(block, "z", 1), after_0])
    down = jnp.stack([shifted(block, "z", -1), after_0])
    landed = [(block[None], ((0, True),)), (up, ((1, True), (0, False))), (down, ((-1, True),))]
    for step in (2, 3):
        up = step_of_ring(up, 1)
        down = step_of_ring(down, -1)
        if step == 2:
            up, text_here = lax.optimization_barrier((up, text_here))
        landed.append((up, ((step, True), (step - 1, False))))
        landed.append((down, ((-step, True), (1 - step, False))))
    up = step_of_ring(up, 1)
    after_3 = step_of_ring(down[1], -1)
    after_4 = step_of_ring(after_3, -1)
    last = [(up, ((4, True), (3, False))), (after_3[None], ((-3, False),))]
    last.append((after_4[None], ((4, False),)))

    column_base = (place - z) * rows
    numbers = jnp.stack([scale, shift_value])
    blocks_of = jnp.arange(z_size, dtype=jnp.int32)
    near_here = blocks_of <= z
    far_here = jnp.full((z_size,), core == 0)
    image_uses = jnp.stack([near_here, far_here, ~near_here, ~far_here], axis=1)
    bases = jnp.stack([column_base, (column_base - 2 * column) % total_rows])

    def matches(piece):
        row = piece[rows].astype(jnp.int32)
        return row[:rows] * rows + row[rows : 2 * rows]

    met = block[:rows]
    met_dunit, met_loss = image_tiles(
        jnp.concatenate([met, block_other[:rows]]),
        jnp.concatenate([matches(block), matches(block_other)])[:, None],
        numbers,
        image_uses.astype(jnp.int32).reshape(-1),
        bases,
        text_here,
        text_before,
    )
    met_loss = met_loss[:rows, 0] + shifted(met_loss[rows:, 0], "core", 1)
    met_dunit = met_dunit[:rows] + shifted(met_dunit[rows:], "core", 1)
    met_low = met.astype(jnp.float32)
    along = jnp.sum(met_low * met_dunit, axis=1)
    across = (met_dunit - met_low * along[:, None]).astype(jnp.float16)
    home = with_rows(across, *digits(along), *digits(met_loss))
    home = shifted_by_window(home, window, 1)
    row_iota = lax.iota(jnp.int32, rows)
    other_place = place + jnp.where(core == 0, z_size, -z_size)
    text_index = jnp.concatenate([place * rows + row_iota, other_place * rows + row_iota])
    text_index = text_index.astype(jnp.float32)[:, None]

    def text_side(group):
        kinds, uses = [], []
        for which, (_, blocks) in enumerate(group):
            for i, (distance, is_here) in enumerate(blocks):
                kinds.append((which, i))
                uses += [((z - distance) % z_size >= z) == is_here, (core == 1) == is_here]
        uses = jnp.stack(uses).astype(jnp.int32)
        return text_tiles(texts, text_index, numbers, uses, [item[0] for item in group], kinds)

    early_dunit = text_side(landed)
    early_dunit, home, last_up = lax.optimization_barrier((early_dunit, home, last[0][0]))
    last[0] = (last_up, last[0][1])
    pair_dunit = early_dunit + text_side(last)
    home = home.astype(jnp.float32)
    tail = home[rows]
    along = tail[:rows] + tail[rows : 2 * rows] * (1.0 / LOW_SCALE)
    row_loss = tail[2 * rows : 3 * rows] + tail[3 * rows : 4 * rows] * (1.0 / LOW_SCALE)
    image_dunit = home[:rows] + image_low.astype(jnp.float32) * along[:, None]
    img_grad = (
        image_dunit - img_unit * jnp.sum(img_unit * image_dunit, axis=1, keepdims=True)
    ) / img_len

    text_dunit = pair_dunit[:rows] + shifted(pair_dunit[rows:], "core", 1)
    txt_grad = (
        text_dunit - txt_unit * jnp.sum(txt_unit * text_dunit, axis=1, keepdims=True)
    ) / txt_len
    return (img_grad, txt_grad, row_loss)


def solution(mesh):
    z_size = mesh.shape["tensor"]
    fine = Mesh(mesh.devices.reshape(-1, 2, z_size), ALL)
    in_specs = (
        P(ROWS_OF, "z"),
        P("z", None),
        P(ALL, None),
        P(ROWS_OF, "z"),
        P("z", None),
        P(),
        P(),
        P(ALL),
        P(),
    )
    out_specs = (P(ALL, None), P(ALL, None), P(ALL))
    return jax.shard_map(body, mesh=fine, in_specs=in_specs, out_specs=out_specs, check_vma=False)
```

```python
import jax
import jax.numpy as jnp
from jax import lax
from jax.experimental import pallas as pl
from jax.experimental.pallas import tpu as pltpu
from jax.sharding import Mesh, PartitionSpec as P


SUM_SCALE = 1024.0
LOW_SCALE = 2048.0
EXTRA = 8
LANES = 128
ROWS_OF = ("chip", "core")
ALL = ("chip", "core", "z")


def shifted(shard, axis, by):
    devices = lax.axis_size(axis)
    return lax.ppermute(shard, axis, [(i, (i + by) % devices) for i in range(devices)])


def step_of_ring(shard, by):
    return shifted(shard, "z", by)


def shifted_by_window(shard, window, sign):
    chips = lax.axis_size("chip")

    def branch(by):
        if by == 0:
            return lambda value: value
        return lambda value: shifted(value, "chip", sign * by)

    return lax.switch(window, [branch(by) for by in range(chips)], shard)


def with_rows(block, *vectors):
    row = jnp.concatenate(vectors)[None, :].astype(block.dtype)
    return jnp.concatenate(
        [block, jnp.pad(row, ((0, EXTRA - 1), (0, block.shape[1] - row.shape[1])))]
    )


def ring_gather(block):
    up = down = block
    found = [block]
    for _ in range(3):
        up = shifted(up, "z", 1)
        down = shifted(down, "z", -1)
        found += [up, down]
    return [*found, shifted(down, "z", -1)]


def ring_sum(parts, z):
    size = parts.shape[0]

    def mine(ahead):
        return lax.dynamic_index_in_dim(parts, (z + ahead) % size, 0, False)

    def sent(up, down):
        up = shifted(up.astype(jnp.float16), "z", 1)
        down = shifted(down.astype(jnp.float16), "z", -1)
        up, down = lax.optimization_barrier((up, down))
        return up.astype(jnp.float32), down.astype(jnp.float32)

    up, down = mine(size // 2), mine(1 - size // 2)
    for ahead in range(size // 2 - 1, 0, -1):
        up, down = sent(up, down)
        up, down = mine(ahead) + up, mine(1 - ahead) + down
    return down + shifted(up.astype(jnp.float16), "z", 1).astype(jnp.float32)


def digits(value):
    high = value.astype(jnp.float16)
    return high, ((value - high.astype(jnp.float32)) * LOW_SCALE).astype(jnp.float16)


def unit_rows(emb):
    length = jnp.sqrt(jnp.sum(emb * emb, axis=1, keepdims=True) + 1e-06)
    return (emb / length, length)


def tile_logits(rows, columns, scale, shift_value):
    cosine = lax.dot_general(
        rows, columns, (((1,), (1,)), ((), ())), preferred_element_type=jnp.float32
    )
    return scale * cosine + shift_value


def used_rows(near, far, rows, count):
    is_near = lax.broadcasted_iota(jnp.int32, (count, 1), 0) < rows
    return jnp.where(is_near, near, far) > 0


def text_tiles(texts, text_index, numbers, uses, stacks, kinds):
    count, width = texts.shape
    rows = count // 2

    def kernel(numbers_ref, uses_ref, texts_ref, index_ref, *refs):
        stack_refs, (near_ref, far_ref) = refs[:-2], refs[-2:]
        scale, shift_value = numbers_ref[0], numbers_ref[1]
        texts_now, index = texts_ref[...], index_ref[...]
        total = jnp.zeros((count, width), jnp.float32)
        for first in range(0, len(kinds), 2):
            columns, match, used = [], [], []
            for at in range(first, min(first + 2, len(kinds))):
                which, i = kinds[at]
                block = stack_refs[which]
                columns.append(block[i, :rows, :])
                digit = block[i, rows : rows + EXTRA, : 2 * rows].astype(jnp.float32)
                match.append(digit[:1, :rows] * rows + digit[:1, rows:])
                near, far = uses_ref[2 * at], uses_ref[2 * at + 1]
                used.append(jnp.broadcast_to(used_rows(near, far, rows, count), (count, rows)))
            columns = jnp.concatenate(columns, axis=0)
            logit = tile_logits(texts_now, columns, scale, shift_value)
            positive = index == jnp.concatenate(match, axis=1)
            coef = (jax.nn.sigmoid(logit) - positive.astype(jnp.float32)) * scale
            coef = jnp.where(jnp.concatenate(used, axis=1), coef, 0.0).astype(jnp.bfloat16)
            total = total + jnp.dot(coef, columns, preferred_element_type=jnp.float32)
        near_ref[...] = total[:rows]
        far_ref[...] = total[rows:]

    work = 4 * count * rows * width * len(kinds)
    return pl.pallas_call(
        kernel,
        out_shape=[jax.ShapeDtypeStruct((rows, width), jnp.float32)] * 2,
        in_specs=[pl.BlockSpec(memory_space=pltpu.SMEM)] * 2
        + [pl.BlockSpec(memory_space=pltpu.VMEM)] * (2 + len(stacks)),
        out_specs=[pl.BlockSpec(memory_space=pltpu.VMEM)] * 2,
        cost_estimate=pl.CostEstimate(flops=work, bytes_accessed=0, transcendentals=0),
        name="text_tiles",
    )(numbers, uses, texts, text_index, *stacks)


def image_tiles(images, image_match, numbers, uses, bases, text_here, text_before):
    count, width = images.shape
    rows = count // 2
    blocks = text_here.shape[0] // rows

    def kernel(
        numbers_ref, uses_ref, bases_ref, images_ref, match_ref, here_ref, before_ref, near_ref,
        far_ref, loss_ref,
    ):
        scale, shift_value = numbers_ref[0], numbers_ref[1]
        images_now, match = images_ref[...], match_ref[...]
        total = jnp.zeros((count, width), jnp.float32)
        loss = jnp.zeros((count, 2 * rows), jnp.float32)
        lane = lax.broadcasted_iota(jnp.int32, (1, rows), 1)
        for at in range(blocks):
            span = pl.ds(at * rows, rows)
            columns = jnp.concatenate([here_ref[span, :], before_ref[span, :]], axis=0)
            index = jnp.concatenate([lane + (bases_ref[i] + at * rows) for i in range(2)], axis=1)
            used = [
                jnp.broadcast_to(
                    used_rows(uses_ref[4 * at + 2 * i], uses_ref[4 * at + 2 * i + 1], rows, count),
                    (count, rows),
                )
                for i in range(2)
            ]
            used = jnp.concatenate(used, axis=1)
            logit = tile_logits(images_now, columns, scale, shift_value)
            positive = match == index
            signed = jnp.where(positive, -logit, logit)
            pair_loss = jnp.maximum(signed, 0.0) + jnp.log1p(jnp.exp(-jnp.abs(signed)))
            loss = loss + jnp.where(used, pair_loss, 0.0)
            coef = (jax.nn.sigmoid(logit) - positive.astype(jnp.float32)) * scale
            coef = jnp.where(used, coef, 0.0).astype(jnp.bfloat16)
            total = total + jnp.dot(coef, columns, preferred_element_type=jnp.float32)
        near_ref[...] = total[:rows]
        far_ref[...] = total[rows:]
        loss_ref[...] = jnp.broadcast_to(jnp.sum(loss, axis=1, keepdims=True), (count, LANES))

    work = 8 * count * rows * width * blocks
    return pl.pallas_call(
        kernel,
        out_shape=(
            jax.ShapeDtypeStruct((rows, width), jnp.float32),
            jax.ShapeDtypeStruct((rows, width), jnp.float32),
            jax.ShapeDtypeStruct((count, LANES), jnp.float32),
        ),
        in_specs=[pl.BlockSpec(memory_space=pltpu.SMEM)] * 3
        + [pl.BlockSpec(memory_space=pltpu.VMEM)] * 4,
        out_specs=[pl.BlockSpec(memory_space=pltpu.VMEM)] * 3,
        cost_estimate=pl.CostEstimate(flops=work, bytes_accessed=0, transcendentals=0),
        name="image_tiles",
    )(numbers, uses, bases, images, image_match, text_here, text_before)


def body(
    img_hidden, img_down, img_pooled, txt_hidden, txt_proj, log_temp, bias, match, window_index
):
    rows, width = img_pooled.shape
    scale = jnp.exp(log_temp[0])
    shift_value = bias[0]
    window = window_index[0]
    place = lax.axis_index(ALL)
    devices = lax.axis_size(ALL)
    z = lax.axis_index("z")
    z_size = lax.axis_size("z")
    core = lax.axis_index("core")
    column = z_size * rows
    total_rows = devices * rows

    img_part = jnp.dot(img_hidden, img_down, preferred_element_type=jnp.float32) * SUM_SCALE
    img_sum = ring_sum(img_part.reshape(z_size, rows, width), z) * (1.0 / SUM_SCALE)

    share = (width + LANES) // 2
    proj_part = jnp.where(core == 0, txt_proj[:, :share], txt_proj[:, width - share :])
    pieces = ring_gather(jnp.concatenate([txt_hidden.T, proj_part], axis=1))

    def joined(part):
        return jnp.concatenate([piece[:, :column] for piece in part])

    here_parts = [joined(pieces[:3]), joined(pieces[3:5])]
    before_parts = [shifted(here, "chip", 1) for here in here_parts]
    img_emb = img_sum + img_pooled.astype(jnp.float32)
    img_unit, img_len = unit_rows(img_emb)
    image_low = img_unit.astype(jnp.bfloat16)
    block = with_rows(image_low, match // rows, match % rows)
    block = shifted_by_window(block, window, -1)
    block, pieces[-1] = lax.optimization_barrier((block, pieces[-1]))
    here_parts.append(joined(pieces[5:]))
    proj_mine = jnp.concatenate([piece[:, column:] for piece in pieces])
    proj_other = shifted(proj_mine, "core", 1)
    proj = jnp.concatenate(
        [
            jnp.where(core == 0, proj_mine, proj_other),
            jnp.where(core == 0, proj_other, proj_mine)[:, 2 * share - width :],
        ],
        axis=1,
    )

    def text_head(hidden_parts):
        emb, row = 0.0, 0
        for hidden in hidden_parts:
            emb = emb + lax.dot_general(
                hidden,
                proj[row : row + hidden.shape[0]],
                (((0,), (0,)), ((), ())),
                preferred_element_type=jnp.float32,
            )
            row += hidden.shape[0]
        return emb

    before_parts.append(shifted(here_parts[2], "chip", 1))
    txt_emb = text_head(here_parts)
    text_here = unit_rows(txt_emb)[0].astype(jnp.bfloat16)
    text_before = unit_rows(text_head(before_parts))[0].astype(jnp.bfloat16)
    txt_unit, txt_len = unit_rows(lax.dynamic_slice_in_dim(txt_emb, z * rows, rows, 0))
    text_low = txt_unit.astype(jnp.bfloat16)
    texts = jnp.concatenate([text_low, shifted(text_low, "core", 1)])

    block_other = shifted(block, "core", 1)

    after_0 = shifted(block, "chip", -1)
    up = jnp.stack([shifted(block, "z", 1), after_0])
    down = jnp.stack([shifted(block, "z", -1), after_0])
    landed = [(block[None], ((0, True),)), (up, ((1, True), (0, False))), (down, ((-1, True),))]
    for step in (2, 3):
        up = step_of_ring(up, 1)
        down = step_of_ring(down, -1)
        if step == 2:
            up, text_here = lax.optimization_barrier((up, text_here))
        landed.append((up, ((step, True), (step - 1, False))))
        landed.append((down, ((-step, True), (1 - step, False))))
    up = step_of_ring(up, 1)
    after_3 = step_of_ring(down[1], -1)
    after_4 = step_of_ring(after_3, -1)
    last = [(up, ((4, True), (3, False))), (after_3[None], ((-3, False),))]
    last.append((after_4[None], ((4, False),)))

    column_base = (place - z) * rows
    numbers = jnp.stack([scale, shift_value])
    blocks_of = jnp.arange(z_size, dtype=jnp.int32)
    near_here = blocks_of <= z
    far_here = jnp.full((z_size,), core == 0)
    image_uses = jnp.stack([near_here, far_here, ~near_here, ~far_here], axis=1)
    bases = jnp.stack([column_base, (column_base - 2 * column) % total_rows])

    def matches(piece):
        row = piece[rows].astype(jnp.int32)
        return row[:rows] * rows + row[rows : 2 * rows]

    met = block[:rows]
    met_near, met_far, met_loss = image_tiles(
        jnp.concatenate([met, block_other[:rows]]),
        jnp.concatenate([matches(block), matches(block_other)])[:, None],
        numbers,
        image_uses.astype(jnp.int32).reshape(-1),
        bases,
        text_here,
        text_before,
    )
    met_loss = met_loss[:rows, 0] + shifted(met_loss[rows:, 0], "core", 1)
    met_dunit = met_near + shifted(met_far, "core", 1)
    met_low = met.astype(jnp.float32)
    along = jnp.sum(met_low * met_dunit, axis=1)
    across = (met_dunit - met_low * along[:, None]).astype(jnp.float16)
    home = with_rows(across, *digits(along), *digits(met_loss))
    home = shifted_by_window(home, window, 1)
    row_iota = lax.iota(jnp.int32, rows)
    other_place = place + jnp.where(core == 0, z_size, -z_size)
    text_index = jnp.concatenate([place * rows + row_iota, other_place * rows + row_iota])
    text_index = text_index.astype(jnp.float32)[:, None]

    def text_side(group):
        kinds, uses = [], []
        for which, (_, blocks) in enumerate(group):
            for i, (distance, is_here) in enumerate(blocks):
                kinds.append((which, i))
                uses += [((z - distance) % z_size >= z) == is_here, (core == 1) == is_here]
        uses = jnp.stack(uses).astype(jnp.int32)
        return text_tiles(texts, text_index, numbers, uses, [item[0] for item in group], kinds)

    early_near, early_far = text_side(landed)
    early_far, home, last_up = lax.optimization_barrier((early_far, home, last[0][0]))
    last[0] = (last_up, last[0][1])
    last_near, last_far = text_side(last)
    home = home.astype(jnp.float32)
    tail = home[rows]
    along = tail[:rows] + tail[rows : 2 * rows] * (1.0 / LOW_SCALE)
    row_loss = tail[2 * rows : 3 * rows] + tail[3 * rows : 4 * rows] * (1.0 / LOW_SCALE)
    image_dunit = home[:rows] + image_low.astype(jnp.float32) * along[:, None]
    img_grad = (
        image_dunit - img_unit * jnp.sum(img_unit * image_dunit, axis=1, keepdims=True)
    ) / img_len

    text_dunit = early_near + last_near + shifted(early_far + last_far, "core", 1)
    txt_grad = (
        text_dunit - txt_unit * jnp.sum(txt_unit * text_dunit, axis=1, keepdims=True)
    ) / txt_len
    return (img_grad, txt_grad, row_loss)


def solution(mesh):
    z_size = mesh.shape["tensor"]
    fine = Mesh(mesh.devices.reshape(-1, 2, z_size), ALL)
    in_specs = (
        P(ROWS_OF, "z"),
        P("z", None),
        P(ALL, None),
        P(ROWS_OF, "z"),
        P("z", None),
        P(),
        P(),
        P(ALL),
        P(),
    )
    out_specs = (P(ALL, None), P(ALL, None), P(ALL))
    return jax.shard_map(body, mesh=fine, in_specs=in_specs, out_specs=out_specs, check_vma=False)
```

```python
import jax
import jax.numpy as jnp
from jax import lax
from jax.experimental import pallas as pl
from jax.experimental.pallas import tpu as pltpu
from jax.sharding import Mesh, PartitionSpec as P


SUM_SCALE = 1024.0
LOW_SCALE = 2048.0
EXTRA = 8
LANES = 128
ROWS_OF = ("chip", "core")
ALL = ("chip", "core", "z")


def shifted(shard, axis, by):
    devices = lax.axis_size(axis)
    return lax.ppermute(shard, axis, [(i, (i + by) % devices) for i in range(devices)])


def step_of_ring(shard, by):
    return shifted(shard, "z", by)


def shifted_by_window(shard, window, sign):
    chips = lax.axis_size("chip")

    def branch(by):
        if by == 0:
            return lambda value: value
        return lambda value: shifted(value, "chip", sign * by)

    return lax.switch(window, [branch(by) for by in range(chips)], shard)


def with_rows(block, *vectors):
    row = jnp.concatenate(vectors)[None, :].astype(block.dtype)
    return jnp.concatenate(
        [block, jnp.pad(row, ((0, EXTRA - 1), (0, block.shape[1] - row.shape[1])))]
    )


def ring_gather(block):
    up = down = block
    found = [block]
    for _ in range(3):
        up = step_of_ring(up, 1)
        down = step_of_ring(down, -1)
        found += [up, down]
    return [*found, shifted(down, "z", -1)]


def ring_sum(parts, z):
    size = parts.shape[0]

    def mine(ahead):
        return lax.dynamic_index_in_dim(parts, (z + ahead) % size, 0, False)

    def sent(up, down):
        up = step_of_ring(up.astype(jnp.float16), 1)
        down = step_of_ring(down.astype(jnp.float16), -1)
        up, down = lax.optimization_barrier((up, down))
        return up.astype(jnp.float32), down.astype(jnp.float32)

    up, down = mine(size // 2), mine(1 - size // 2)
    for ahead in range(size // 2 - 1, 0, -1):
        up, down = sent(up, down)
        up, down = mine(ahead) + up, mine(1 - ahead) + down
    return down + shifted(up.astype(jnp.float16), "z", 1).astype(jnp.float32)


def digits(value):
    high = value.astype(jnp.float16)
    return high, ((value - high.astype(jnp.float32)) * LOW_SCALE).astype(jnp.float16)


def unit_rows(emb):
    length = jnp.sqrt(jnp.sum(emb * emb, axis=1, keepdims=True) + 1e-06)
    return (emb / length, length)


def tile_logits(rows, columns, scale, shift_value):
    cosine = lax.dot_general(
        rows, columns, (((1,), (1,)), ((), ())), preferred_element_type=jnp.float32
    )
    return scale * cosine + shift_value


def used_rows(near, far, rows, count):
    is_near = lax.broadcasted_iota(jnp.int32, (count, 1), 0) < rows
    return jnp.where(is_near, near, far) > 0


def text_tiles(texts, text_index, numbers, uses, stacks, kinds):
    count, width = texts.shape
    rows = count // 2

    def kernel(numbers_ref, uses_ref, texts_ref, index_ref, *refs):
        stack_refs, (near_ref, far_ref) = refs[:-2], refs[-2:]
        scale, shift_value = numbers_ref[0], numbers_ref[1]
        texts_now, index = texts_ref[...], index_ref[...]
        total = jnp.zeros((count, width), jnp.float32)
        for first in range(0, len(kinds), 2):
            columns, match, used = [], [], []
            for at in range(first, min(first + 2, len(kinds))):
                which, i = kinds[at]
                block = stack_refs[which]
                columns.append(block[i, :rows, :])
                digit = block[i, rows : rows + EXTRA, : 2 * rows].astype(jnp.float32)
                match.append(digit[:1, :rows] * rows + digit[:1, rows:])
                near, far = uses_ref[2 * at], uses_ref[2 * at + 1]
                used.append(jnp.broadcast_to(used_rows(near, far, rows, count), (count, rows)))
            columns = jnp.concatenate(columns, axis=0)
            logit = tile_logits(texts_now, columns, scale, shift_value)
            positive = index == jnp.concatenate(match, axis=1)
            coef = (jax.nn.sigmoid(logit) - positive.astype(jnp.float32)) * scale
            coef = jnp.where(jnp.concatenate(used, axis=1), coef, 0.0).astype(jnp.bfloat16)
            total = total + jnp.dot(coef, columns, preferred_element_type=jnp.float32)
        near_ref[...] = total[:rows]
        far_ref[...] = total[rows:]

    work = 4 * count * rows * width * len(kinds)
    return pl.pallas_call(
        kernel,
        out_shape=[jax.ShapeDtypeStruct((rows, width), jnp.float32)] * 2,
        in_specs=[pl.BlockSpec(memory_space=pltpu.SMEM)] * 2
        + [pl.BlockSpec(memory_space=pltpu.VMEM)] * (2 + len(stacks)),
        out_specs=[pl.BlockSpec(memory_space=pltpu.VMEM)] * 2,
        cost_estimate=pl.CostEstimate(flops=work, bytes_accessed=0, transcendentals=0),
        name="text_tiles",
    )(numbers, uses, texts, text_index, *stacks)


def image_tiles(images, image_match, numbers, uses, bases, text_here, text_before):
    count, width = images.shape
    rows = count // 2
    blocks = text_here.shape[0] // rows

    def kernel(
        numbers_ref, uses_ref, bases_ref, images_ref, match_ref, here_ref, before_ref, near_ref,
        far_ref, loss_ref,
    ):
        scale, shift_value = numbers_ref[0], numbers_ref[1]
        images_now, match = images_ref[...], match_ref[...]
        total = jnp.zeros((count, width), jnp.float32)
        loss = jnp.zeros((count, 2 * rows), jnp.float32)
        lane = lax.broadcasted_iota(jnp.int32, (1, rows), 1)
        for at in range(blocks):
            span = pl.ds(at * rows, rows)
            columns = jnp.concatenate([here_ref[span, :], before_ref[span, :]], axis=0)
            index = jnp.concatenate([lane + (bases_ref[i] + at * rows) for i in range(2)], axis=1)
            used = [
                jnp.broadcast_to(
                    used_rows(uses_ref[4 * at + 2 * i], uses_ref[4 * at + 2 * i + 1], rows, count),
                    (count, rows),
                )
                for i in range(2)
            ]
            used = jnp.concatenate(used, axis=1)
            logit = tile_logits(images_now, columns, scale, shift_value)
            positive = match == index
            signed = jnp.where(positive, -logit, logit)
            pair_loss = jnp.maximum(signed, 0.0) + jnp.log1p(jnp.exp(-jnp.abs(signed)))
            loss = loss + jnp.where(used, pair_loss, 0.0)
            coef = (jax.nn.sigmoid(logit) - positive.astype(jnp.float32)) * scale
            coef = jnp.where(used, coef, 0.0).astype(jnp.bfloat16)
            total = total + jnp.dot(coef, columns, preferred_element_type=jnp.float32)
        near_ref[...] = total[:rows]
        far_ref[...] = total[rows:]
        loss_ref[...] = jnp.broadcast_to(jnp.sum(loss, axis=1, keepdims=True), (count, LANES))

    work = 8 * count * rows * width * blocks
    return pl.pallas_call(
        kernel,
        out_shape=(
            jax.ShapeDtypeStruct((rows, width), jnp.float32),
            jax.ShapeDtypeStruct((rows, width), jnp.float32),
            jax.ShapeDtypeStruct((count, LANES), jnp.float32),
        ),
        in_specs=[pl.BlockSpec(memory_space=pltpu.SMEM)] * 3
        + [pl.BlockSpec(memory_space=pltpu.VMEM)] * 4,
        out_specs=[pl.BlockSpec(memory_space=pltpu.VMEM)] * 3,
        cost_estimate=pl.CostEstimate(flops=work, bytes_accessed=0, transcendentals=0),
        name="image_tiles",
    )(numbers, uses, bases, images, image_match, text_here, text_before)


def body(
    img_hidden, img_down, img_pooled, txt_hidden, txt_proj, log_temp, bias, match, window_index
):
    rows, width = img_pooled.shape
    scale = jnp.exp(log_temp[0])
    shift_value = bias[0]
    window = window_index[0]
    place = lax.axis_index(ALL)
    devices = lax.axis_size(ALL)
    z = lax.axis_index("z")
    z_size = lax.axis_size("z")
    core = lax.axis_index("core")
    column = z_size * rows
    total_rows = devices * rows

    img_part = jnp.dot(img_hidden, img_down, preferred_element_type=jnp.float32) * SUM_SCALE
    img_sum = ring_sum(img_part.reshape(z_size, rows, width), z) * (1.0 / SUM_SCALE)

    share = (width + LANES) // 2
    proj_part = jnp.where(core == 0, txt_proj[:, :share], txt_proj[:, width - share :])
    pieces = ring_gather(jnp.concatenate([txt_hidden.T, proj_part], axis=1))

    def joined(part):
        return jnp.concatenate([piece[:, :column] for piece in part])

    here_parts = [joined(pieces[:3]), joined(pieces[3:5])]
    before_parts = [shifted(here, "chip", 1) for here in here_parts]
    img_emb = img_sum + img_pooled.astype(jnp.float32)
    img_unit, img_len = unit_rows(img_emb)
    image_low = img_unit.astype(jnp.bfloat16)
    block = with_rows(image_low, match // rows, match % rows)
    block = shifted_by_window(block, window, -1)
    block, pieces[-1] = lax.optimization_barrier((block, pieces[-1]))
    here_parts.append(joined(pieces[5:]))
    proj_mine = jnp.concatenate([piece[:, column:] for piece in pieces])
    proj_other = shifted(proj_mine, "core", 1)
    proj = jnp.concatenate(
        [
            jnp.where(core == 0, proj_mine, proj_other),
            jnp.where(core == 0, proj_other, proj_mine)[:, 2 * share - width :],
        ],
        axis=1,
    )

    def text_head(hidden_parts):
        emb, row = 0.0, 0
        for hidden in hidden_parts:
            emb = emb + lax.dot_general(
                hidden,
                proj[row : row + hidden.shape[0]],
                (((0,), (0,)), ((), ())),
                preferred_element_type=jnp.float32,
            )
            row += hidden.shape[0]
        return emb

    before_parts.append(shifted(here_parts[2], "chip", 1))
    txt_emb = text_head(here_parts)
    text_here = unit_rows(txt_emb)[0].astype(jnp.bfloat16)
    text_before = unit_rows(text_head(before_parts))[0].astype(jnp.bfloat16)
    txt_unit, txt_len = unit_rows(lax.dynamic_slice_in_dim(txt_emb, z * rows, rows, 0))
    text_low = txt_unit.astype(jnp.bfloat16)
    texts = jnp.concatenate([text_low, shifted(text_low, "core", 1)])

    block_other = shifted(block, "core", 1)

    after_0 = shifted(block, "chip", -1)
    up = jnp.stack([shifted(block, "z", 1), after_0])
    down = jnp.stack([shifted(block, "z", -1), after_0])
    landed = [(block[None], ((0, True),)), (up, ((1, True), (0, False))), (down, ((-1, True),))]
    for step in (2, 3):
        up = step_of_ring(up, 1)
        down = step_of_ring(down, -1)
        if step == 2:
            up, text_here = lax.optimization_barrier((up, text_here))
        landed.append((up, ((step, True), (step - 1, False))))
        landed.append((down, ((-step, True), (1 - step, False))))
    up = step_of_ring(up, 1)
    after_3 = step_of_ring(down[1], -1)
    after_4 = step_of_ring(after_3, -1)
    last = [(up, ((4, True), (3, False))), (after_3[None], ((-3, False),))]
    last.append((after_4[None], ((4, False),)))

    column_base = (place - z) * rows
    numbers = jnp.stack([scale, shift_value])
    blocks_of = jnp.arange(z_size, dtype=jnp.int32)
    near_here = blocks_of <= z
    far_here = jnp.full((z_size,), core == 0)
    image_uses = jnp.stack([near_here, far_here, ~near_here, ~far_here], axis=1)
    bases = jnp.stack([column_base, (column_base - 2 * column) % total_rows])

    def matches(piece):
        row = piece[rows].astype(jnp.int32)
        return row[:rows] * rows + row[rows : 2 * rows]

    met = block[:rows]
    met_near, met_far, met_loss = image_tiles(
        jnp.concatenate([met, block_other[:rows]]),
        jnp.concatenate([matches(block), matches(block_other)])[:, None],
        numbers,
        image_uses.astype(jnp.int32).reshape(-1),
        bases,
        text_here,
        text_before,
    )
    met_loss = met_loss[:rows, 0] + shifted(met_loss[rows:, 0], "core", 1)
    met_dunit = met_near + shifted(met_far, "core", 1)
    met_low = met.astype(jnp.float32)
    along = jnp.sum(met_low * met_dunit, axis=1)
    across = (met_dunit - met_low * along[:, None]).astype(jnp.float16)
    home = with_rows(across, *digits(along), *digits(met_loss))
    home = shifted_by_window(home, window, 1)
    row_iota = lax.iota(jnp.int32, rows)
    other_place = place + jnp.where(core == 0, z_size, -z_size)
    text_index = jnp.concatenate([place * rows + row_iota, other_place * rows + row_iota])
    text_index = text_index.astype(jnp.float32)[:, None]

    def text_side(group):
        kinds, uses = [], []
        for which, (_, blocks) in enumerate(group):
            for i, (distance, is_here) in enumerate(blocks):
                kinds.append((which, i))
                uses += [((z - distance) % z_size >= z) == is_here, (core == 1) == is_here]
        uses = jnp.stack(uses).astype(jnp.int32)
        return text_tiles(texts, text_index, numbers, uses, [item[0] for item in group], kinds)

    early_near, early_far = text_side(landed)
    early_far, home, last_up = lax.optimization_barrier((early_far, home, last[0][0]))
    last[0] = (last_up, last[0][1])
    last_near, last_far = text_side(last)
    home = home.astype(jnp.float32)
    tail = home[rows]
    along = tail[:rows] + tail[rows : 2 * rows] * (1.0 / LOW_SCALE)
    row_loss = tail[2 * rows : 3 * rows] + tail[3 * rows : 4 * rows] * (1.0 / LOW_SCALE)
    image_dunit = home[:rows] + image_low.astype(jnp.float32) * along[:, None]
    img_grad = (
        image_dunit - img_unit * jnp.sum(img_unit * image_dunit, axis=1, keepdims=True)
    ) / img_len

    text_dunit = early_near + last_near + shifted(early_far + last_far, "core", 1)
    txt_grad = (
        text_dunit - txt_unit * jnp.sum(txt_unit * text_dunit, axis=1, keepdims=True)
    ) / txt_len
    return (img_grad, txt_grad, row_loss)


def solution(mesh):
    z_size = mesh.shape["tensor"]
    fine = Mesh(mesh.devices.reshape(-1, 2, z_size), ALL)
    in_specs = (
        P(ROWS_OF, "z"),
        P("z", None),
        P(ALL, None),
        P(ROWS_OF, "z"),
        P("z", None),
        P(),
        P(),
        P(ALL),
        P(),
    )
    out_specs = (P(ALL, None), P(ALL, None), P(ALL))
    return jax.shard_map(body, mesh=fine, in_specs=in_specs, out_specs=out_specs, check_vma=False)
```
